128 devices in a mesh: row: 4 (over z_hi, core), col: 8 (over z_lo, x), depth: 4 (over y).
Axes of the slice: x: 4, y: 4, z: 4 (z_hi: 2, z_lo: 2; z = z_hi * 2 + z_lo), core: 2. Of those that a mesh axis runs over, the one named last changes fastest.
Arguments:
- pair_input: bfloat16 [768, 768, 128], P('row', ('col', 'depth')), may hold values from -40 to 40
- in_gain: float32 [128], replicated, may hold values from 0.1 to 1.9
- in_shift: float32 [128], replicated, may hold values from -3 to 3
- w_proj: bfloat16 [128, 512], replicated, may hold values from -0.5 to 0.5
- w_gate: bfloat16 [128, 128], replicated, may hold values from -0.5 to 0.5
- out_gain: float32 [128], replicated, may hold values from 0.1 to 1.9
- out_shift: float32 [128], replicated, may hold values from -3 to 3
- w_out: bfloat16 [128, 128], replicated, may hold values from -0.5 to 0.5
Outputs:
- update: bfloat16 [768, 768, 128], P('row', ('col', 'depth'))
The draws below stay inside these ranges and needn't reach their ends.
All inputs are finite; a program needn't handle non-finite values.
Results may differ from the reference program's by a relative error of at most 0.013.
Values may be sent and summed in bfloat16 or wider, within the bound.
A program may use at most 64 MiB of HBM per device.

```python
import math
import jax
import jax.numpy as jnp
from jax import lax

C_Z = 128
C = 128
RESIDUES = 768


def draw_pair_input(key, part):
    key_entries = jax.random.fold_in(key, 11)
    key_scales = jax.random.fold_in(key, 12)
    scales = jnp.exp(jax.random.uniform(key_scales, (RESIDUES, RESIDUES, 1), jnp.float32, 0.0, math.log(10.0)))
    entries = jnp.clip(jax.random.normal(key_entries, (RESIDUES, RESIDUES, C_Z), jnp.float32), -4.0, 4.0)
    values = entries * scales
    return values.astype(jnp.bfloat16)


def gaussian(stream_key, shape, width, most, kind=jnp.bfloat16):
    return jnp.clip(width * jax.random.normal(stream_key, shape, jnp.float32), -most, most).astype(kind)


def setup_inputs(seed: int = 0) -> dict:
    splits = jax.random.split(jax.random.key(seed), 9)
    return {
        "pair_input": draw_pair_input(jax.random.fold_in(splits[8], 71), 0),
        "in_gain": jnp.clip(1.0 + 0.18 * jax.random.normal(splits[1], (C_Z,), jnp.float32), 0.1, 1.9),
        "in_shift": gaussian(splits[2], (C_Z,), 0.5, 3.0, jnp.float32),
        "w_proj": gaussian(splits[3], (C_Z, 4 * C), C_Z ** -0.5, 0.5),
        "w_gate": gaussian(splits[4], (C_Z, C_Z), C_Z ** -0.5, 0.5),
        "out_gain": jnp.clip(1.0 + 0.18 * jax.random.normal(splits[5], (C,), jnp.float32), 0.1, 1.9),
        "out_shift": gaussian(splits[6], (C,), 0.5, 3.0, jnp.float32),
        "w_out": gaussian(splits[7], (C, C_Z), C ** -0.5, 0.5),
    }


def layer_norm(values, scaling, offsets):
    average = lax.optimization_barrier(jnp.mean(values, axis=-1, keepdims=True))
    centred = values - average
    variance = lax.optimization_barrier(jnp.mean(centred * centred, axis=-1, keepdims=True))
    return centred * lax.rsqrt(variance + 1e-05) * scaling + offsets

def reference(pair_input, in_gain, in_shift, w_proj, w_gate, out_gain, out_shift, w_out):
    normed = layer_norm(pair_input.astype(jnp.float32), in_gain, in_shift).astype(jnp.bfloat16)
    channels = w_proj.shape[1] // 4

    def side_rows(normed_row):
        projected = jnp.dot(normed_row, w_proj, preferred_element_type=jnp.float32)
        left_side = (jax.nn.sigmoid(projected[:, :channels]) * projected[:, channels:2 * channels]).astype(jnp.bfloat16)
        right_side = (jax.nn.sigmoid(projected[:, 2 * channels:3 * channels]) * projected[:, 3 * channels:]).astype(jnp.bfloat16)
        return (left_side, right_side)
    left_side, right_side = lax.map(side_rows, normed)
    product = jnp.einsum('kic,kjc->ijc', left_side.astype(jnp.float32), right_side.astype(jnp.float32), precision=lax.Precision.HIGHEST)
    product_norm = layer_norm(product, out_gain, out_shift).astype(jnp.bfloat16)
    gating = jax.nn.sigmoid(jnp.einsum('xyc,cd->xyd', normed.astype(jnp.float32), w_gate.astype(jnp.float32), precision=lax.Precision.HIGHEST))
    projected_out = jnp.einsum('xyc,cd->xyd', product_norm.astype(jnp.float32), w_out.astype(jnp.float32), precision=lax.Precision.HIGHEST)
    return (gating * projected_out).astype(jnp.bfloat16)
```

```python
import functools

import jax
import jax.numpy as jnp
from jax import lax
from jax.experimental import pallas as pl
from jax.experimental.pallas import tpu as pltpu
from jax.sharding import PartitionSpec as P

BF = jnp.bfloat16
F32 = jnp.float32
EPS = 1e-05


def div(a, b):
    return lax.div(a, jnp.int32(b))


def rem(a, b):
    return lax.rem(a, jnp.int32(b))


def dot_nt(a, b):
    return lax.dot_general(a, b, (((1,), (1,)), ((), ())), preferred_element_type=F32)


def kernel(
    x_ref, ig_ref, is_ref, wp_ref, wg_ref, og_ref, os_ref, wo_ref, out_ref,
    xin, xs, wsel, lsend, rsend, stage, recv_l, recv_r, psend, recv_p, peer_p,
    gate, pn, ostage, obf,
    own_sem, x_send, x_recv, l_send, l_recv, r_send, r_recv, p_send, p_recv, e_send, e_recv, o_sem,
):
    row = lax.axis_index("row")
    col = lax.axis_index("col")
    y = lax.axis_index("depth")
    zh, core = div(row, 2), rem(row, 2)
    zl, x = div(col, 4), rem(col, 4)
    q = col * 4 + y
    me = zh * 32 + q
    other = {"row": zh * 2 + 1 - core, "col": col, "depth": y}
    low = pl.multiple_of(zh * 384, 128)

    def chip(o):
        zh2 = rem(zh + div(o, 32), 2)
        zl2 = rem(zl + div(o, 16), 2)
        x2 = rem(x + div(o, 4), 4)
        y2 = rem(y + o, 4)
        col2 = zl2 * 4 + x2
        q2 = col2 * 4 + y2
        return zh2, q2, zh2 * 32 + q2, {"row": zh2 * 2 + core, "col": col2, "depth": y2}

    def own_copy(t, u):
        start = core * 128 + u * 64 if u < 2 else 256 + core * 64
        return pltpu.make_async_copy(
            x_ref.at[:, u, :, pl.ds(t * 8, 8), :], xin.at[t, pl.ds(div(start, 8), 8)], own_sem.at[t]
        )

    for t in range(3):
        for u in range(3):
            own_copy(t, u).start()

    barrier = pltpu.get_barrier_semaphore()
    pl.semaphore_signal(barrier, inc=1, device_id=other)

    def greet(o, carry):
        pl.semaphore_signal(barrier, inc=1, device_id=chip(o)[3])
        return carry

    lax.fori_loop(1, 64, greet, 0)

    for part in range(4):
        block = wp_ref[:, part * 128 : (part + 1) * 128].astype(F32).T
        stage[0, 0:128, :] = block
        wsel[part * 64 : (part + 1) * 64, :] = stage[0, pl.ds(pl.multiple_of(core * 64, 64), 64), :].astype(BF)

    pl.semaphore_wait(barrier, 64)

    def peer_copy(t, u):
        start = core * 128 + u * 64 if u < 2 else 256 + core * 64
        return pltpu.make_async_remote_copy(
            src_ref=x_ref.at[:, u, :, pl.ds(t * 8, 8), :],
            dst_ref=xin.at[t, pl.ds(div(start, 8), 8)],
            send_sem=x_send,
            recv_sem=x_recv.at[t],
            device_id=other,
        )

    for t in range(3):
        for u in range(3):
            peer_copy(t, u).start()

    in_gain = ig_ref[...]
    in_shift = is_ref[...]

    def norm_rows(t):
        def chunk(i, carry):
            v = xin[t, pl.ds(i * 4, 4)].astype(F32)
            v = v - jnp.mean(v, axis=-1, keepdims=True)
            v = v * lax.rsqrt(jnp.mean(v * v, axis=-1, keepdims=True) + EPS)
            v = v * in_gain.reshape(1, 1, 1, 128) + in_shift.reshape(1, 1, 1, 128)
            xs[pl.ds(pl.multiple_of(t * 3072 + i * 256, 256), 256), :] = v.reshape(256, 128)
            return carry

        lax.fori_loop(0, 12, chunk, 0)

    def project(t, base, dst):
        w = wsel[base : base + 128, :]
        for i in range(8):
            rows = xs[pl.ds(t * 3072 + i, 384, stride=8), :].astype(BF)
            p = dot_nt(w, rows)
            side = jax.nn.sigmoid(p[0:64]) * p[64:128]
            for c in range(3):
                stage[c, pl.ds(i, 64, stride=8), :] = side[:, c * 128 : (c + 1) * 128]
        for c in range(3):
            dst[pl.ds(t * 64, 64), :, c * 128 : (c + 1) * 128] = stage[c].reshape(64, 8, 128).astype(BF)

    def left(t, carry):
        pltpu.make_async_copy(xin.at[t, pl.ds(0, 24)], xin.at[t, pl.ds(0, 24)], own_sem.at[t]).wait()
        pltpu.make_async_copy(xin.at[t, pl.ds(0, 24)], xin.at[t, pl.ds(0, 24)], x_recv.at[t]).wait()
        norm_rows(t)
        project(t, 0, lsend)
        late = div(t, 2)
        group = div(q, 16) * 48 + rem(div(q, 8), 2) * (16 - 8 * late) + t * 8 * (1 - late) + 32 * late + rem(q, 8)

        def send(o, carry):
            _, _, n, device = chip(o)
            pltpu.make_async_remote_copy(
                src_ref=lsend.at[t * 64 + n],
                dst_ref=recv_l.at[group, :, pl.ds(low, 384)],
                send_sem=l_send,
                recv_sem=l_recv,
                device_id=device,
            ).start()
            return carry

        lax.fori_loop(1, 64, send, 0)
        recv_l[group, :, pl.ds(low, 384)] = lsend[t * 64 + me]
        return carry

    lax.fori_loop(0, 3, left, 0)

    def right(t, carry):
        project(t, 128, rsend)

        def send(o, carry):
            _, _, n, device = chip(o)
            pltpu.make_async_remote_copy(
                src_ref=rsend.at[t * 64 + n],
                dst_ref=recv_r.at[t * 32 + q, :, pl.ds(low, 384)],
                send_sem=r_send,
                recv_sem=r_recv.at[t],
                device_id=device,
            ).start()
            return carry

        lax.fori_loop(1, 64, send, 0)
        recv_r[t * 32 + q, :, pl.ds(low, 384)] = rsend[t * 64 + me]
        return carry

    lax.fori_loop(0, 3, right, 0)

    def gates(t, carry):
        w = wg_ref[...]
        for i in range(8):
            a = xs[pl.ds(t * 3072 + core * 1024 + i, 128, stride=8), :].astype(BF)
            b = xs[pl.ds(t * 3072 + 2048 + core * 512 + i, 64, stride=8), :].astype(BF)
            rows = jnp.concatenate([a, b], axis=0)
            gate[t * 8 + i] = jax.nn.sigmoid(jnp.dot(rows, w, preferred_element_type=F32))
        return carry

    lax.fori_loop(0, 3, gates, 0)

    pltpu.make_async_copy(lsend.at[pl.ds(0, 189)], lsend.at[pl.ds(0, 189)], l_recv).wait()

    def product(t, carry):
        pltpu.make_async_copy(rsend.at[pl.ds(0, 63)], rsend.at[pl.ds(0, 63)], r_recv.at[t]).wait()
        rows = recv_r[pl.ds(t * 32, 32)].reshape(256, 768)
        for part in range(3):
            cols = recv_l[pl.ds(part * 32, 32)].reshape(256, 768)
            psend[pl.ds(t * 32, 32), :, part * 256 : (part + 1) * 256] = (
                dot_nt(rows, cols).astype(BF).reshape(32, 8, 256)
            )

        def send(o, carry):
            zh2, q2, _, device = chip(o)
            pltpu.make_async_remote_copy(
                src_ref=psend.at[t * 32 + q2, :, pl.ds(pl.multiple_of(zh2 * 384, 128), 384)],
                dst_ref=recv_p.at[t * 64 + me],
                send_sem=p_send,
                recv_sem=p_recv.at[t],
                device_id=device,
            ).start()
            return carry

        lax.fori_loop(1, 64, send, 0)
        recv_p[t * 64 + me] = psend[t * 32 + q, :, pl.ds(low, 384)]
        return carry

    lax.fori_loop(0, 3, product, 0)

    def to_peer(t, half):
        lane = pl.multiple_of((1 - core) * 128, 128) if half == 0 else 256
        return pltpu.make_async_remote_copy(
            src_ref=recv_p.at[pl.ds(t * 64, 64), :, pl.ds(lane, 128)],
            dst_ref=peer_p.at[pl.ds(t * 64, 64), :, pl.ds(half * 128, 128)],
            send_sem=e_send,
            recv_sem=e_recv.at[t],
            device_id=other,
        )

    own_lane = pl.multiple_of(core * 128, 128)
    first = core == 0
    out_gain = jnp.where(first, og_ref[...], pltpu.roll(og_ref[...], 64, 1))
    out_shift = jnp.where(first, os_ref[...], pltpu.roll(os_ref[...], 64, 1))

    def out_copy(t, u):
        return pltpu.make_async_copy(
            obf.at[pl.ds(u * 8, 8), :, pl.ds(t * 8, 8), :], out_ref.at[:, u, :, pl.ds(t * 8, 8), :], o_sem
        )

    def finish(t, carry):
        pltpu.make_async_copy(rsend.at[pl.ds(0, 63)], rsend.at[pl.ds(0, 63)], p_recv.at[t]).wait()
        to_peer(t, 0).start()
        to_peer(t, 1).start()
        pltpu.make_async_copy(
            peer_p.at[pl.ds(0, 64)], peer_p.at[pl.ds(0, 64)], e_recv.at[t]
        ).wait()

        def parts(lo, size):
            here = pl.ds(t * 64 + lo, size)
            return (
                jnp.concatenate(
                    [recv_p[here, :, pl.ds(own_lane, 128)], recv_p[here, :, 256:384]], axis=-1
                ).astype(F32),
                peer_p[here].astype(F32),
            )

        total = jnp.zeros((8, 256), F32)
        for lo in range(0, 64, 16):
            a, b = parts(lo, 16)
            total = total + (jnp.sum(a, axis=0) + jnp.sum(b, axis=0))
        average = total * (1.0 / 128.0)
        total = jnp.zeros((8, 256), F32)
        for lo in range(0, 64, 16):
            a, b = parts(lo, 16)
            a, b = a - average[None], b - average[None]
            total = total + (jnp.sum(a * a, axis=0) + jnp.sum(b * b, axis=0))
        scale = lax.rsqrt(total * (1.0 / 128.0) + EPS)
        for lo in range(0, 64, 16):
            a, b = parts(lo, 16)
            a = ((a - average[None]) * scale[None]).reshape(128, 256)
            b = ((b - average[None]) * scale[None]).reshape(128, 256)
            for c in range(2):
                pn[c, lo * 8 : lo * 8 + 128, :] = a[:, c * 128 : (c + 1) * 128]
                pn[c, 512 + lo * 8 : 512 + lo * 8 + 128, :] = b[:, c * 128 : (c + 1) * 128]
        w_own = wo_ref[pl.ds(pl.multiple_of(core * 64, 64), 64), :]
        w_other = wo_ref[pl.ds(pl.multiple_of((1 - core) * 64, 64), 64), :]
        w = jnp.concatenate([w_own, w_other], axis=0)
        for j in range(8):
            a = pn[0, pl.ds(j, 128, stride=8), :].T
            b = pn[1, pl.ds(j, 128, stride=8), :].T
            v = jnp.concatenate([a, jnp.where(first, b[0:64], b[64:128])], axis=0)
            v = (v * out_gain + out_shift).astype(BF)
            u = jnp.dot(v, w, preferred_element_type=F32) * gate[t * 8 + j]
            ostage[pl.ds(j, 192, stride=8), :] = u
        obf[:, :, pl.ds(t * 8, 8), :] = ostage[...].reshape(24, 8, 8, 128).astype(BF)
        for u in range(3):
            out_copy(t, u).start()
        return carry

    lax.fori_loop(0, 3, finish, 0)

    for t in range(3):
        for u in range(3):
            out_copy(t, u).wait()
            peer_copy(t, u).wait_send()
        to_peer(t, 0).wait_send()
        to_peer(t, 1).wait_send()
    for sem, buf in ((l_send, lsend), (r_send, rsend), (p_send, recv_p)):
        pltpu.make_async_copy(buf.at[pl.ds(0, 189)], buf.at[pl.ds(0, 189)], sem).wait()


def per_device(pair_input, in_gain, in_shift, w_proj, w_gate, out_gain, out_shift, w_out):
    vmem = pl.BlockSpec(memory_space=pltpu.VMEM)
    anyspace = pl.BlockSpec(memory_space=pl.ANY)
    dma = pltpu.SemaphoreType.DMA
    out = pl.pallas_call(
        kernel,
        out_shape=jax.ShapeDtypeStruct((8, 3, 8, 24, 128), BF),
        in_specs=[anyspace] + [vmem] * 7,
        out_specs=anyspace,
        scratch_shapes=[
            pltpu.VMEM((3, 48, 8, 8, 128), BF),
            pltpu.VMEM((9216, 128), F32),
            pltpu.VMEM((256, 128), BF),
            pltpu.VMEM((192, 8, 384), BF),
            pltpu.VMEM((192, 8, 384), BF),
            pltpu.VMEM((3, 512, 128), F32),
            pltpu.VMEM((96, 8, 768), BF),
            pltpu.VMEM((96, 8, 768), BF),
            pltpu.VMEM((96, 8, 768), BF),
            pltpu.VMEM((192, 8, 384), BF),
            pltpu.VMEM((192, 8, 256), BF),
            pltpu.VMEM((24, 192, 128), F32),
            pltpu.VMEM((2, 1024, 128), F32),
            pltpu.VMEM((1536, 128), F32),
            pltpu.VMEM((24, 8, 24, 128), BF),
            dma((3,)),
            dma,
            dma((3,)),
            dma,
            dma,
            dma,
            dma((3,)),
            dma,
            dma((3,)),
            dma,
            dma((3,)),
            dma,
        ],
        compiler_params=pltpu.CompilerParams(
            collective_id=0, has_side_effects=True, vmem_limit_bytes=56 * 2**20
        ),
        name="triangle",
    )(
        pair_input.reshape(8, 3, 8, 24, 128),
        in_gain.reshape(1, 128),
        in_shift.reshape(1, 128),
        w_proj,
        w_gate,
        out_gain.reshape(1, 128),
        out_shift.reshape(1, 128),
        w_out,
    )
    return out.reshape(192, 24, 128)


def solution(mesh):
    placed = (P("row", ("col", "depth"), None), P(), P(), P(), P(), P(), P(), P())
    return jax.shard_map(
        per_device,
        mesh=mesh,
        in_specs=placed,
        out_specs=P("row", ("col", "depth"), None),
        check_vma=False,
    )
```

```python
import itertools

import jax
import jax.numpy as jnp
from jax import lax
from jax.experimental import pallas as pl
from jax.experimental.pallas import tpu as pltpu
from jax.sharding import PartitionSpec as P

BF = jnp.bfloat16
F32 = jnp.float32
EPS = 1e-05


def div(a, b):
    return lax.div(a, jnp.int32(b))


def rem(a, b):
    return lax.rem(a, jnp.int32(b))


def dot_nt(a, b):
    return lax.dot_general(a, b, (((1,), (1,)), ((), ())), preferred_element_type=F32)


def hops(step):
    dzh, dzl, dx, dy = step
    return (2 if dzh else 0) + dzl + min(dx, 4 - dx) + min(dy, 4 - dy)


ORDER = [(1, 0, 2, 2), (0, 1, 2, 2), (0, 1, 0, 0), (1, 1, 2, 2), (1, 1, 0, 0), (1, 0, 1, 2), (0, 0, 3, 0), (1, 0, 2, 1), (0, 0, 0, 3), (1, 0, 2, 3), (0, 0, 0, 1), (1, 0, 3, 2), (0, 0, 1, 0), (0, 1, 1, 2), (0, 1, 3, 0), (0, 1, 2, 1), (0, 1, 0, 3), (0, 1, 2, 3), (0, 1, 0, 1), (0, 1, 3, 2), (0, 1, 1, 0), (1, 1, 1, 2), (1, 1, 3, 0), (1, 1, 2, 1), (1, 1, 0, 3), (1, 1, 2, 3), (1, 1, 0, 1), (1, 1, 3, 2), (1, 1, 1, 0), (0, 1, 0, 2), (0, 1, 2, 0), (0, 1, 1, 1), (0, 1, 3, 3), (0, 1, 1, 3), (0, 1, 3, 1), (1, 1, 0, 2), (1, 1, 2, 0), (1, 1, 1, 1), (1, 1, 3, 3), (1, 1, 1, 3), (1, 1, 3, 1), (0, 0, 2, 2), (1, 0, 0, 0), (1, 0, 0, 2), (0, 0, 2, 0), (1, 0, 1, 1), (0, 0, 3, 3), (1, 0, 1, 3), (0, 0, 3, 1), (1, 0, 2, 0), (0, 0, 0, 2), (1, 0, 3, 1), (0, 0, 1, 3), (1, 0, 3, 3), (0, 0, 1, 1), (0, 0, 1, 2), (1, 0, 3, 0), (0, 0, 2, 1), (1, 0, 0, 3), (0, 0, 2, 3), (1, 0, 0, 1), (0, 0, 3, 2), (1, 0, 1, 0)]


def kernel(
    x_ref, ig_ref, is_ref, wp_ref, wg_ref, og_ref, os_ref, wo_ref, out_ref,
    xin, xs, wsel, lsend, rsend, stage, recv_l, recv_r, psend, recv_p, peer_p,
    gate, pn, ostage, wp, wg, wo, vecs,
    w_sem, own_sem, x_send, x_recv, l_send, l_recv, r_send, r_recv, p_send, p_recv, e_send, e_recv,
):
    row = lax.axis_index("row")
    col = lax.axis_index("col")
    y = lax.axis_index("depth")
    zh, core = div(row, 2), rem(row, 2)
    zl, x = div(col, 4), rem(col, 4)
    q = col * 4 + y
    me = zh * 32 + q
    other = {"row": zh * 2 + 1 - core, "col": col, "depth": y}
    low = pl.multiple_of(zh * 384, 128)

    rows2 = [(zh, row), (1 - zh, (1 - zh) * 2 + core)]
    xs2 = [rem(x + d, 4) for d in range(4)]
    cols2 = [[a * 4 + b for b in xs2] for a in (zl, 1 - zl)]
    ys2 = [rem(y + d, 4) for d in range(4)]

    def each_chip(use):
        for dzh, dzl, dx, dy in ORDER:
            zh2, row2 = rows2[dzh]
            q2 = cols2[dzl][dx] * 4 + ys2[dy]
            use(zh2, q2, zh2 * 32 + q2, {"row": row2, "col": cols2[dzl][dx], "depth": ys2[dy]})

    weights = [
        pltpu.make_async_copy(src, dst, w_sem.at[n])
        for n, (src, dst) in enumerate(
            ((wp_ref, wp), (ig_ref, vecs.at[0]), (is_ref, vecs.at[1]), (wg_ref, wg), (og_ref, vecs.at[2]),
             (os_ref, vecs.at[3]), (wo_ref, wo))
        )
    ]

    def own_copy(t, u):
        start = core * 128 + u * 64 if u < 2 else 256 + core * 64
        return pltpu.make_async_copy(
            x_ref.at[:, u, :, pl.ds(t * 8, 8), :], xin.at[t, pl.ds(div(start, 8), 8)], own_sem.at[t]
        )

    for t in range(3):
        for u in range(3):
            own_copy(t, u).start()
    for copy in weights:
        copy.start()

    barrier = pltpu.get_barrier_semaphore()
    each_chip(lambda zh2, q2, n, device: pl.semaphore_signal(barrier, inc=1, device_id=device))
    pl.semaphore_signal(barrier, inc=1, device_id=other)

    for copy in weights:
        copy.wait()
    for part in range(4):
        block = wp[:, part * 128 : (part + 1) * 128].astype(F32).T
        stage[0, 0:128, :] = block
        wsel[part * 64 : (part + 1) * 64, :] = stage[0, pl.ds(pl.multiple_of(core * 64, 64), 64), :].astype(BF)

    in_gain = vecs[0]
    in_shift = vecs[1]
    mean_of = jnp.full((128, 128), 1.0 / 128.0, BF)
    mean_of_two = jnp.full((256, 128), 1.0 / 128.0, BF)

    def norm_own(t, carry):
        pltpu.make_async_copy(xin.at[t, pl.ds(0, 24)], xin.at[t, pl.ds(0, 24)], own_sem.at[t]).wait()
        for n in range(6):
            start = core * 16 + n * 4 if n < 4 else 32 + core * 8 + (n - 4) * 4
            raw = xin[t, pl.ds(start, 4)].reshape(256, 128)
            v = raw.astype(F32) - jnp.dot(raw, mean_of, preferred_element_type=F32)
            square = v * v
            upper = square.astype(BF)
            lower = (square - upper.astype(F32)).astype(BF)
            variance = jnp.dot(
                jnp.concatenate([upper, lower], axis=1), mean_of_two, preferred_element_type=F32
            )
            v = v * lax.rsqrt(variance + EPS) * in_gain + in_shift
            xs[pl.ds(pl.multiple_of(t * 3072 + start * 64, 256), 256), :] = v
            xin[t, pl.ds(start, 4)] = v.astype(BF).reshape(4, 8, 8, 128)
        return carry

    lax.fori_loop(0, 3, norm_own, 0)

    pl.semaphore_wait(barrier, 64)

    def peer_copy(t, u):
        here = pl.ds(core * 16, 16) if u == 0 else pl.ds(32 + core * 8, 8)
        return pltpu.make_async_remote_copy(
            src_ref=xin.at[t, here],
            dst_ref=xin.at[t, here],
            send_sem=x_send,
            recv_sem=x_recv.at[t],
            device_id=other,
        )

    for t in range(3):
        for u in range(2):
            peer_copy(t, u).start()

    def widen_peer(t):
        for n in range(6):
            start = (1 - core) * 16 + n * 4 if n < 4 else 32 + (1 - core) * 8 + (n - 4) * 4
            xs[pl.ds(pl.multiple_of(t * 3072 + start * 64, 256), 256), :] = (
                xin[t, pl.ds(start, 4)].reshape(256, 128).astype(F32)
            )

    def project(t, base, dst):
        w = wsel[base : base + 128, :]
        for i in range(8):
            rows = xs[pl.ds(t * 3072 + i, 384, stride=8), :].astype(BF)
            p = dot_nt(w, rows)
            side = jax.nn.sigmoid(p[0:64]) * p[64:128]
            for c in range(3):
                stage[c, pl.ds(i, 64, stride=8), :] = side[:, c * 128 : (c + 1) * 128]
        for c in range(3):
            dst[pl.ds(t * 64, 64), :, c * 128 : (c + 1) * 128] = stage[c].reshape(64, 8, 128).astype(BF)

    def left(t, carry):
        pltpu.make_async_copy(xin.at[t, pl.ds(0, 24)], xin.at[t, pl.ds(0, 24)], x_recv.at[t]).wait()
        widen_peer(t)
        project(t, 0, lsend)
        late = div(t, 2)
        group = div(q, 16) * 48 + rem(div(q, 8), 2) * (16 - 8 * late) + t * 8 * (1 - late) + 32 * late + rem(q, 8)

        def send(zh2, q2, n, device):
            pltpu.make_async_remote_copy(
                src_ref=lsend.at[t * 64 + n],
                dst_ref=recv_l.at[group, :, pl.ds(low, 384)],
                send_sem=l_send,
                recv_sem=l_recv,
                device_id=device,
            ).start()

        each_chip(send)
        recv_l[group, :, pl.ds(low, 384)] = lsend[t * 64 + me]
        return carry

    lax.fori_loop(0, 3, left, 0)

    def right(t, carry):
        project(t, 128, rsend)

        def send(zh2, q2, n, device):
            pltpu.make_async_remote_copy(
                src_ref=rsend.at[t * 64 + n],
                dst_ref=recv_r.at[t * 32 + q, :, pl.ds(low, 384)],
                send_sem=r_send,
                recv_sem=r_recv.at[t],
                device_id=device,
            ).start()

        each_chip(send)
        recv_r[t * 32 + q, :, pl.ds(low, 384)] = rsend[t * 64 + me]
        return carry

    lax.fori_loop(0, 3, right, 0)

    def gates(t, carry):
        w = wg[...]
        for i in range(8):
            a = xs[pl.ds(t * 3072 + core * 1024 + i, 128, stride=8), :].astype(BF)
            b = xs[pl.ds(t * 3072 + 2048 + core * 512 + i, 64, stride=8), :].astype(BF)
            rows = jnp.concatenate([a, b], axis=0)
            gate[t * 8 + i] = jax.nn.sigmoid(jnp.dot(rows, w, preferred_element_type=F32))
        return carry

    lax.fori_loop(0, 3, gates, 0)

    pltpu.make_async_copy(lsend.at[pl.ds(0, 189)], lsend.at[pl.ds(0, 189)], l_recv).wait()

    def product(t, carry):
        pltpu.make_async_copy(rsend.at[pl.ds(0, 63)], rsend.at[pl.ds(0, 63)], r_recv.at[t]).wait()
        rows = recv_r[pl.ds(t * 32, 32)].reshape(256, 768)
        for part in range(3):
            cols = recv_l[pl.ds(part * 32, 32)].reshape(256, 768)
            psend[pl.ds(t * 32, 32), :, part * 256 : (part + 1) * 256] = (
                dot_nt(rows, cols).astype(BF).reshape(32, 8, 256)
            )

        def send(zh2, q2, n, device):
            pltpu.make_async_remote_copy(
                src_ref=psend.at[t * 32 + q2, :, pl.ds(pl.multiple_of(zh2 * 384, 128), 384)],
                dst_ref=recv_p.at[t * 64 + me],
                send_sem=p_send,
                recv_sem=p_recv.at[t],
                device_id=device,
            ).start()

        each_chip(send)
        recv_p[t * 64 + me] = psend[t * 32 + q, :, pl.ds(low, 384)]
        return carry

    lax.fori_loop(0, 3, product, 0)

    def to_peer(t, half):
        lane = pl.multiple_of((1 - core) * 128, 128) if half == 0 else 256
        return pltpu.make_async_remote_copy(
            src_ref=recv_p.at[pl.ds(t * 64, 64), :, pl.ds(lane, 128)],
            dst_ref=peer_p.at[pl.ds(t * 64, 64), :, pl.ds(half * 128, 128)],
            send_sem=e_send,
            recv_sem=e_recv.at[t],
            device_id=other,
        )

    own_lane = pl.multiple_of(core * 128, 128)
    first = core == 0
    out_gain = jnp.where(first, vecs[2], pltpu.roll(vecs[2], 64, 1))
    out_shift = jnp.where(first, vecs[3], pltpu.roll(vecs[3], 64, 1))

    def finish(t, carry):
        pltpu.make_async_copy(rsend.at[pl.ds(0, 63)], rsend.at[pl.ds(0, 63)], p_recv.at[t]).wait()
        to_peer(t, 0).start()
        to_peer(t, 1).start()
        pltpu.make_async_copy(
            peer_p.at[pl.ds(0, 64)], peer_p.at[pl.ds(0, 64)], e_recv.at[t]
        ).wait()

        def parts(lo, size):
            here = pl.ds(t * 64 + lo, size)
            return (
                jnp.concatenate(
                    [recv_p[here, :, pl.ds(own_lane, 128)], recv_p[here, :, 256:384]], axis=-1
                ).astype(F32),
                peer_p[here].astype(F32),
            )

        total = jnp.zeros((8, 256), F32)
        for lo in range(0, 64, 16):
            a, b = parts(lo, 16)
            total = total + (jnp.sum(a, axis=0) + jnp.sum(b, axis=0))
        average = total * (1.0 / 128.0)
        total = jnp.zeros((8, 256), F32)
        for lo in range(0, 64, 16):
            a, b = parts(lo, 16)
            a, b = a - average[None], b - average[None]
            total = total + (jnp.sum(a * a, axis=0) + jnp.sum(b * b, axis=0))
        scale = lax.rsqrt(total * (1.0 / 128.0) + EPS)
        for lo in range(0, 64, 16):
            a, b = parts(lo, 16)
            a = ((a - average[None]) * scale[None]).reshape(128, 256)
            b = ((b - average[None]) * scale[None]).reshape(128, 256)
            for c in range(2):
                pn[c, lo * 8 : lo * 8 + 128, :] = a[:, c * 128 : (c + 1) * 128]
                pn[c, 512 + lo * 8 : 512 + lo * 8 + 128, :] = b[:, c * 128 : (c + 1) * 128]
        w_own = wo[pl.ds(pl.multiple_of(core * 64, 64), 64), :]
        w_other = wo[pl.ds(pl.multiple_of((1 - core) * 64, 64), 64), :]
        w = jnp.concatenate([w_own, w_other], axis=0)
        for j in range(8):
            a = pn[0, pl.ds(j, 128, stride=8), :].T
            b = pn[1, pl.ds(j, 128, stride=8), :].T
            v = jnp.concatenate([a, jnp.where(first, b[0:64], b[64:128])], axis=0)
            v = (v * out_gain + out_shift).astype(BF)
            u = jnp.dot(v, w, preferred_element_type=F32) * gate[t * 8 + j]
            ostage[pl.ds(j, 192, stride=8), :] = u
        for u in range(3):
            out_ref[:, u, :, pl.ds(pl.multiple_of(t * 8, 8), 8), :] = (
                ostage[u * 512 : (u + 1) * 512, :].reshape(8, 8, 8, 128).astype(BF)
            )
        return carry

    lax.fori_loop(0, 3, finish, 0)

    for t in range(3):
        for u in range(2):
            peer_copy(t, u).wait_send()
        to_peer(t, 0).wait_send()
        to_peer(t, 1).wait_send()
    for sem, buf in ((l_send, lsend), (r_send, rsend), (p_send, recv_p)):
        pltpu.make_async_copy(buf.at[pl.ds(0, 189)], buf.at[pl.ds(0, 189)], sem).wait()


def per_device(pair_input, in_gain, in_shift, w_proj, w_gate, out_gain, out_shift, w_out):
    vmem = pl.BlockSpec(memory_space=pltpu.VMEM)
    anyspace = pl.BlockSpec(memory_space=pltpu.HBM)
    dma = pltpu.SemaphoreType.DMA
    out = pl.pallas_call(
        kernel,
        out_shape=pltpu.VMEM((8, 3, 8, 24, 128), BF),
        in_specs=[anyspace] * 8,
        out_specs=vmem,
        scratch_shapes=[
            pltpu.VMEM((3, 48, 8, 8, 128), BF),
            pltpu.VMEM((9216, 128), F32),
            pltpu.VMEM((256, 128), BF),
            pltpu.VMEM((192, 8, 384), BF),
            pltpu.VMEM((192, 8, 384), BF),
            pltpu.VMEM((3, 512, 128), F32),
            pltpu.VMEM((96, 8, 768), BF),
            pltpu.VMEM((96, 8, 768), BF),
            pltpu.VMEM((96, 8, 768), BF),
            pltpu.VMEM((192, 8, 384), BF),
            pltpu.VMEM((192, 8, 256), BF),
            pltpu.VMEM((24, 192, 128), F32),
            pltpu.VMEM((2, 1024, 128), F32),
            pltpu.VMEM((1536, 128), F32),
            pltpu.VMEM((128, 512), BF),
            pltpu.VMEM((128, 128), BF),
            pltpu.VMEM((128, 128), BF),
            pltpu.VMEM((4, 1, 128), F32),
            dma((7,)),
            dma((3,)),
            dma,
            dma((3,)),
            dma,
            dma,
            dma,
            dma((3,)),
            dma,
            dma((3,)),
            dma,
            dma((3,)),
        ],
        compiler_params=pltpu.CompilerParams(
            collective_id=0, has_side_effects=True, vmem_limit_bytes=int(54 * 2**20)
        ),
        name="triangle",
    )(
        *(
            pltpu.with_memory_space_constraint(a, pltpu.HBM)
            for a in (
                pair_input.reshape(8, 3, 8, 24, 128),
                in_gain.reshape(1, 128),
                in_shift.reshape(1, 128),
                w_proj,
                w_gate,
                out_gain.reshape(1, 128),
                out_shift.reshape(1, 128),
                w_out,
            )
        )
    )
    return out.reshape(192, 24, 128)


def solution(mesh):
    placed = (P("row", ("col", "depth"), None), P(), P(), P(), P(), P(), P(), P())
    return jax.shard_map(
        per_device,
        mesh=mesh,
        in_specs=placed,
        out_specs=P("row", ("col", "depth"), None),
        check_vma=False,
    )
```

```python
import itertools

import jax
import jax.numpy as jnp
from jax import lax
from jax.experimental import pallas as pl
from jax.experimental.pallas import tpu as pltpu
from jax.sharding import PartitionSpec as P

BF = jnp.bfloat16
F32 = jnp.float32
EPS = 1e-05


def div(a, b):
    return lax.div(a, jnp.int32(b))


def rem(a, b):
    return lax.rem(a, jnp.int32(b))


def dot_nt(a, b):
    return lax.dot_general(a, b, (((1,), (1,)), ((), ())), preferred_element_type=F32)


def hops(step):
    dzh, dzl, dx, dy = step
    return (2 if dzh else 0) + dzl + min(dx, 4 - dx) + min(dy, 4 - dy)


ORDER = [(1, 0, 2, 2), (0, 1, 2, 2), (0, 1, 0, 0), (1, 1, 2, 2), (1, 1, 0, 0), (1, 0, 1, 2), (0, 0, 3, 0), (1, 0, 2, 1), (0, 0, 0, 3), (1, 0, 2, 3), (0, 0, 0, 1), (1, 0, 3, 2), (0, 0, 1, 0), (0, 1, 1, 2), (0, 1, 3, 0), (0, 1, 2, 1), (0, 1, 0, 3), (0, 1, 2, 3), (0, 1, 0, 1), (0, 1, 3, 2), (0, 1, 1, 0), (1, 1, 1, 2), (1, 1, 3, 0), (1, 1, 2, 1), (1, 1, 0, 3), (1, 1, 2, 3), (1, 1, 0, 1), (1, 1, 3, 2), (1, 1, 1, 0), (0, 1, 0, 2), (0, 1, 2, 0), (0, 1, 1, 1), (0, 1, 3, 3), (0, 1, 1, 3), (0, 1, 3, 1), (1, 1, 0, 2), (1, 1, 2, 0), (1, 1, 1, 1), (1, 1, 3, 3), (1, 1, 1, 3), (1, 1, 3, 1), (0, 0, 2, 2), (1, 0, 0, 0), (1, 0, 0, 2), (0, 0, 2, 0), (1, 0, 1, 1), (0, 0, 3, 3), (1, 0, 1, 3), (0, 0, 3, 1), (1, 0, 2, 0), (0, 0, 0, 2), (1, 0, 3, 1), (0, 0, 1, 3), (1, 0, 3, 3), (0, 0, 1, 1), (0, 0, 1, 2), (1, 0, 3, 0), (0, 0, 2, 1), (1, 0, 0, 3), (0, 0, 2, 3), (1, 0, 0, 1), (0, 0, 3, 2), (1, 0, 1, 0)]


FAR = sorted(ORDER, key=lambda s: -hops(s))


def kernel(
    x_ref, ig_ref, is_ref, wp_ref, wg_ref, og_ref, os_ref, wo_ref, out_ref,
    xin, xs, wall, lown, lsend, rsend, stage, recv_l, recv_r, psend, recv_p, peer_p,
    gate, pn, ostage, wp, wg, wo, vecs,
    w_sem, own_sem, x_send, x_recv, l_send, l_recv, r_send, r_recv, p_send, p_recv, e_send, e_recv,
):
    row = lax.axis_index("row")
    col = lax.axis_index("col")
    y = lax.axis_index("depth")
    zh, core = div(row, 2), rem(row, 2)
    zl, x = div(col, 4), rem(col, 4)
    q = col * 4 + y
    me = zh * 32 + q
    other = {"row": zh * 2 + 1 - core, "col": col, "depth": y}
    low = pl.multiple_of(zh * 384, 128)

    rows2 = [(zh, row, zh * 2 + 1 - core), (1 - zh, (1 - zh) * 2 + core, (1 - zh) * 2 + 1 - core)]
    xs2 = [rem(x + d, 4) for d in range(4)]
    cols2 = [[a * 4 + b for b in xs2] for a in (zl, 1 - zl)]
    ys2 = [rem(y + d, 4) for d in range(4)]

    def each_chip(use, order=ORDER):
        for dzh, dzl, dx, dy in order:
            zh2, row2, _ = rows2[dzh]
            q2 = cols2[dzl][dx] * 4 + ys2[dy]
            use(zh2, q2, zh2 * 32 + q2, {"row": row2, "col": cols2[dzl][dx], "depth": ys2[dy]})

    def each_device(use, order):
        for dzh, dzl, dx, dy in order:
            zh2, row2, cross2 = rows2[dzh]
            n = zh2 * 32 + cols2[dzl][dx] * 4 + ys2[dy]
            use(n, core, {"row": row2, "col": cols2[dzl][dx], "depth": ys2[dy]})
            use(n, 1 - core, {"row": cross2, "col": cols2[dzl][dx], "depth": ys2[dy]})
        use(me, 1 - core, other)

    weights = [
        pltpu.make_async_copy(src, dst, w_sem.at[n])
        for n, (src, dst) in enumerate(
            ((wp_ref, wp), (ig_ref, vecs.at[0]), (is_ref, vecs.at[1]), (wg_ref, wg), (og_ref, vecs.at[2]),
             (os_ref, vecs.at[3]), (wo_ref, wo))
        )
    ]

    def own_copy(t, u):
        start = core * 128 + u * 64 if u < 2 else 256 + core * 64
        return pltpu.make_async_copy(
            x_ref.at[:, u, :, pl.ds(t * 8, 8), :], xin.at[t, pl.ds(div(start, 8), 8)], own_sem.at[t]
        )

    for t in range(3):
        for u in range(3):
            own_copy(t, u).start()
    for copy in weights:
        copy.start()

    barrier = pltpu.get_barrier_semaphore()
    each_device(lambda n, owner, device: pl.semaphore_signal(barrier, inc=1, device_id=device), FAR)

    for copy in weights:
        copy.wait()
    for part in range(4):
        wall[part * 128 : (part + 1) * 128, :] = wp[:, part * 128 : (part + 1) * 128].astype(F32).T.astype(BF)

    in_gain = vecs[0]
    in_shift = vecs[1]
    mean_of = jnp.full((128, 128), 1.0 / 128.0, BF)
    mean_of_two = jnp.full((256, 128), 1.0 / 128.0, BF)

    def norm_own(t, carry):
        pltpu.make_async_copy(xin.at[t, pl.ds(0, 24)], xin.at[t, pl.ds(0, 24)], own_sem.at[t]).wait()
        for n in range(6):
            start = core * 16 + n * 4 if n < 4 else 32 + core * 8 + (n - 4) * 4
            raw = xin[t, pl.ds(start, 4)].reshape(256, 128)
            v = raw.astype(F32) - jnp.dot(raw, mean_of, preferred_element_type=F32)
            square = v * v
            upper = square.astype(BF)
            lower = (square - upper.astype(F32)).astype(BF)
            variance = jnp.dot(
                jnp.concatenate([upper, lower], axis=1), mean_of_two, preferred_element_type=F32
            )
            v = v * lax.rsqrt(variance + EPS) * in_gain + in_shift
            xs[pl.ds(pl.multiple_of(t * 3072 + start * 64, 256), 256), :] = v
            xin[t, pl.ds(start, 4)] = v.astype(BF).reshape(4, 8, 8, 128)
        return carry

    def group_of(t):
        late = div(t, 2)
        return div(q, 16) * 48 + rem(div(q, 8), 2) * (16 - 8 * late) + t * 8 * (1 - late) + 32 * late + rem(q, 8)

    norm_own(0, 0)
    for i in range(8):
        rows = xs[pl.ds(core * 1024 + i, 128, stride=8), :].astype(BF)
        p = dot_nt(wall[0:256, :], rows)
        pn[0, pl.ds(i, 128, stride=8), :] = jax.nn.sigmoid(p[0:128]) * p[128:256]
    lown[...] = pn[0].reshape(128, 8, 128).astype(BF)
    lax.fori_loop(1, 3, norm_own, 0)

    pl.semaphore_wait(barrier, 127)

    def peer_copy(t, u):
        here = pl.ds(core * 16, 16) if u == 0 else pl.ds(32 + core * 8, 8)
        return pltpu.make_async_remote_copy(
            src_ref=xin.at[t, here],
            dst_ref=xin.at[t, here],
            send_sem=x_send,
            recv_sem=x_recv.at[t],
            device_id=other,
        )

    for t in range(3):
        for u in range(2):
            peer_copy(t, u).start()

    own_tile = pl.ds(pl.multiple_of(zh * 384 + core * 128, 128), 128)
    group = group_of(jnp.int32(0))

    def send_own(n, owner, device):
        pltpu.make_async_remote_copy(
            src_ref=lown.at[owner * 64 + n],
            dst_ref=recv_l.at[group, :, own_tile],
            send_sem=l_send,
            recv_sem=l_recv,
            device_id=device,
        ).start()

    each_device(send_own, ORDER)
    recv_l[group, :, own_tile] = lown[core * 64 + me]

    def widen_peer(t):
        for n in range(6):
            start = (1 - core) * 16 + n * 4 if n < 4 else 32 + (1 - core) * 8 + (n - 4) * 4
            xs[pl.ds(pl.multiple_of(t * 3072 + start * 64, 256), 256), :] = (
                xin[t, pl.ds(start, 4)].reshape(256, 128).astype(F32)
            )

    def project(t, base, dst, tiles):
        w = jnp.concatenate(
            [wall[pl.ds(pl.multiple_of(part * 128 + core * 64, 64), 64), :] for part in (base, base + 1)], axis=0
        )
        for i in range(8):
            rows = xs[pl.ds(t * 3072 + tiles[0] * 1024 + i, len(tiles) * 128, stride=8), :].astype(BF)
            p = dot_nt(w, rows)
            side = jax.nn.sigmoid(p[0:64]) * p[64:128]
            for n, c in enumerate(tiles):
                stage[c, pl.ds(i, 64, stride=8), :] = side[:, n * 128 : (n + 1) * 128]
        for c in tiles:
            dst[pl.ds(t * 64, 64), :, c * 128 : (c + 1) * 128] = stage[c].reshape(64, 8, 128).astype(BF)

    def left(t, tiles):
        pltpu.make_async_copy(xin.at[t, pl.ds(0, 24)], xin.at[t, pl.ds(0, 24)], x_recv.at[t]).wait()
        widen_peer(t)
        project(t, 0, lsend, tiles)
        group = group_of(t)
        size = len(tiles) * 128
        src_lanes = pl.ds(tiles[0] * 128, size)
        dst_lanes = pl.ds(pl.multiple_of(low + tiles[0] * 128, 128), size)

        def send(zh2, q2, n, device):
            pltpu.make_async_remote_copy(
                src_ref=lsend.at[t * 64 + n, :, src_lanes],
                dst_ref=recv_l.at[group, :, dst_lanes],
                send_sem=l_send,
                recv_sem=l_recv,
                device_id=device,
            ).start()

        each_chip(send)
        recv_l[group, :, dst_lanes] = lsend[t * 64 + me, :, src_lanes]

    left(jnp.int32(0), (2,))

    def left_all(t, carry):
        left(t, (0, 1, 2))
        return carry

    lax.fori_loop(1, 3, left_all, 0)

    def right(t, carry):
        project(t, 2, rsend, (0, 1, 2))

        def send(zh2, q2, n, device):
            pltpu.make_async_remote_copy(
                src_ref=rsend.at[t * 64 + n],
                dst_ref=recv_r.at[t * 32 + q, :, pl.ds(low, 384)],
                send_sem=r_send,
                recv_sem=r_recv.at[t],
                device_id=device,
            ).start()

        each_chip(send)
        recv_r[t * 32 + q, :, pl.ds(low, 384)] = rsend[t * 64 + me]
        return carry

    lax.fori_loop(0, 3, right, 0)

    def gates(t, carry):
        w = wg[...]
        for i in range(8):
            a = xs[pl.ds(t * 3072 + core * 1024 + i, 128, stride=8), :].astype(BF)
            b = xs[pl.ds(t * 3072 + 2048 + core * 512 + i, 64, stride=8), :].astype(BF)
            rows = jnp.concatenate([a, b], axis=0)
            gate[t * 8 + i] = jax.nn.sigmoid(jnp.dot(rows, w, preferred_element_type=F32))
        return carry

    lax.fori_loop(0, 3, gates, 0)

    pltpu.make_async_copy(xs.at[pl.ds(0, 2272)], xs.at[pl.ds(0, 2272)], l_recv).wait()

    def product(t, carry):
        pltpu.make_async_copy(rsend.at[pl.ds(0, 63)], rsend.at[pl.ds(0, 63)], r_recv.at[t]).wait()
        rows = recv_r[pl.ds(t * 32, 32)].reshape(256, 768)
        for part in range(3):
            cols = recv_l[pl.ds(part * 32, 32)].reshape(256, 768)
            psend[pl.ds(t * 32, 32), :, part * 256 : (part + 1) * 256] = (
                dot_nt(rows, cols).astype(BF).reshape(32, 8, 256)
            )

        def send(zh2, q2, n, device):
            pltpu.make_async_remote_copy(
                src_ref=psend.at[t * 32 + q2, :, pl.ds(pl.multiple_of(zh2 * 384, 128), 384)],
                dst_ref=recv_p.at[t * 64 + me],
                send_sem=p_send,
                recv_sem=p_recv.at[t],
                device_id=device,
            ).start()

        each_chip(send)
        recv_p[t * 64 + me] = psend[t * 32 + q, :, pl.ds(low, 384)]
        return carry

    lax.fori_loop(0, 3, product, 0)

    def to_peer(t, half):
        lane = pl.multiple_of((1 - core) * 128, 128) if half == 0 else 256
        return pltpu.make_async_remote_copy(
            src_ref=recv_p.at[pl.ds(t * 64, 64), :, pl.ds(lane, 128)],
            dst_ref=peer_p.at[pl.ds(t * 64, 64), :, pl.ds(half * 128, 128)],
            send_sem=e_send,
            recv_sem=e_recv.at[t],
            device_id=other,
        )

    own_lane = pl.multiple_of(core * 128, 128)
    first = core == 0
    out_gain = jnp.where(first, vecs[2], pltpu.roll(vecs[2], 64, 1))
    out_shift = jnp.where(first, vecs[3], pltpu.roll(vecs[3], 64, 1))

    def finish(t, carry):
        pltpu.make_async_copy(rsend.at[pl.ds(0, 63)], rsend.at[pl.ds(0, 63)], p_recv.at[t]).wait()
        to_peer(t, 0).start()
        to_peer(t, 1).start()
        pltpu.make_async_copy(
            peer_p.at[pl.ds(0, 64)], peer_p.at[pl.ds(0, 64)], e_recv.at[t]
        ).wait()

        def parts(lo, size):
            here = pl.ds(t * 64 + lo, size)
            return (
                jnp.concatenate(
                    [recv_p[here, :, pl.ds(own_lane, 128)], recv_p[here, :, 256:384]], axis=-1
                ).astype(F32),
                peer_p[here].astype(F32),
            )

        total = jnp.zeros((8, 256), F32)
        for lo in range(0, 64, 16):
            a, b = parts(lo, 16)
            total = total + (jnp.sum(a, axis=0) + jnp.sum(b, axis=0))
        average = total * (1.0 / 128.0)
        total = jnp.zeros((8, 256), F32)
        for lo in range(0, 64, 16):
            a, b = parts(lo, 16)
            a, b = a - average[None], b - average[None]
            total = total + (jnp.sum(a * a, axis=0) + jnp.sum(b * b, axis=0))
        scale = lax.rsqrt(total * (1.0 / 128.0) + EPS)
        for lo in range(0, 64, 16):
            a, b = parts(lo, 16)
            a = ((a - average[None]) * scale[None]).reshape(128, 256)
            b = ((b - average[None]) * scale[None]).reshape(128, 256)
            for c in range(2):
                pn[c, lo * 8 : lo * 8 + 128, :] = a[:, c * 128 : (c + 1) * 128]
                pn[c, 512 + lo * 8 : 512 + lo * 8 + 128, :] = b[:, c * 128 : (c + 1) * 128]
        w_own = wo[pl.ds(pl.multiple_of(core * 64, 64), 64), :]
        w_other = wo[pl.ds(pl.multiple_of((1 - core) * 64, 64), 64), :]
        w = jnp.concatenate([w_own, w_other], axis=0)
        for j in range(8):
            a = pn[0, pl.ds(j, 128, stride=8), :].T
            b = pn[1, pl.ds(j, 128, stride=8), :].T
            v = jnp.concatenate([a, jnp.where(first, b[0:64], b[64:128])], axis=0)
            v = (v * out_gain + out_shift).astype(BF)
            u = jnp.dot(v, w, preferred_element_type=F32) * gate[t * 8 + j]
            ostage[pl.ds(j, 192, stride=8), :] = u
        for u in range(3):
            out_ref[:, u, :, pl.ds(pl.multiple_of(t * 8, 8), 8), :] = (
                ostage[u * 512 : (u + 1) * 512, :].reshape(8, 8, 8, 128).astype(BF)
            )
        return carry

    lax.fori_loop(0, 3, finish, 0)

    for t in range(3):
        for u in range(2):
            peer_copy(t, u).wait_send()
        to_peer(t, 0).wait_send()
        to_peer(t, 1).wait_send()
    pltpu.make_async_copy(xs.at[pl.ds(0, 2272)], xs.at[pl.ds(0, 2272)], l_send).wait()
    for sem, buf in ((r_send, rsend), (p_send, recv_p)):
        pltpu.make_async_copy(buf.at[pl.ds(0, 189)], buf.at[pl.ds(0, 189)], sem).wait()


def per_device(pair_input, in_gain, in_shift, w_proj, w_gate, out_gain, out_shift, w_out):
    vmem = pl.BlockSpec(memory_space=pltpu.VMEM)
    anyspace = pl.BlockSpec(memory_space=pltpu.HBM)
    dma = pltpu.SemaphoreType.DMA
    out = pl.pallas_call(
        kernel,
        out_shape=pltpu.VMEM((8, 3, 8, 24, 128), BF),
        in_specs=[anyspace] * 8,
        out_specs=vmem,
        scratch_shapes=[
            pltpu.VMEM((3, 48, 8, 8, 128), BF),
            pltpu.VMEM((9216, 128), F32),
            pltpu.VMEM((512, 128), BF),
            pltpu.VMEM((128, 8, 128), BF),
            pltpu.VMEM((192, 8, 384), BF),
            pltpu.VMEM((192, 8, 384), BF),
            pltpu.VMEM((3, 512, 128), F32),
            pltpu.VMEM((96, 8, 768), BF),
            pltpu.VMEM((96, 8, 768), BF),
            pltpu.VMEM((96, 8, 768), BF),
            pltpu.VMEM((192, 8, 384), BF),
            pltpu.VMEM((192, 8, 256), BF),
            pltpu.VMEM((24, 192, 128), F32),
            pltpu.VMEM((2, 1024, 128), F32),
            pltpu.VMEM((1536, 128), F32),
            pltpu.VMEM((128, 512), BF),
            pltpu.VMEM((128, 128), BF),
            pltpu.VMEM((128, 128), BF),
            pltpu.VMEM((4, 1, 128), F32),
            dma((7,)),
            dma((3,)),
            dma,
            dma((3,)),
            dma,
            dma,
            dma,
            dma((3,)),
            dma,
            dma((3,)),
            dma,
            dma((3,)),
        ],
        compiler_params=pltpu.CompilerParams(
            collective_id=0, has_side_effects=True, vmem_limit_bytes=int(54 * 2**20)
        ),
        name="triangle",
    )(
        *(
            pltpu.with_memory_space_constraint(a, pltpu.HBM)
            for a in (
                pair_input.reshape(8, 3, 8, 24, 128),
                in_gain.reshape(1, 128),
                in_shift.reshape(1, 128),
                w_proj,
                w_gate,
                out_gain.reshape(1, 128),
                out_shift.reshape(1, 128),
                w_out,
            )
        )
    )
    return out.reshape(192, 24, 128)


def solution(mesh):
    placed = (P("row", ("col", "depth"), None), P(), P(), P(), P(), P(), P(), P())
    return jax.shard_map(
        per_device,
        mesh=mesh,
        in_specs=placed,
        out_specs=P("row", ("col", "depth"), None),
        check_vma=False,
    )
```

```python
import itertools

import jax
import jax.numpy as jnp
from jax import lax
from jax.experimental import pallas as pl
from jax.experimental.pallas import tpu as pltpu
from jax.sharding import PartitionSpec as P

BF = jnp.bfloat16
F32 = jnp.float32
EPS = 1e-05


def div(a, b):
    return lax.div(a, jnp.int32(b))


def rem(a, b):
    return lax.rem(a, jnp.int32(b))


def dot_nt(a, b):
    return lax.dot_general(a, b, (((1,), (1,)), ((), ())), preferred_element_type=F32)


def hops(step):
    dzh, dzl, dx, dy = step
    return (2 if dzh else 0) + dzl + min(dx, 4 - dx) + min(dy, 4 - dy)


ORDER = [(1, 0, 2, 2), (0, 1, 2, 2), (0, 1, 0, 0), (1, 1, 2, 2), (1, 1, 0, 0), (1, 0, 1, 2), (0, 0, 3, 0), (1, 0, 2, 1), (0, 0, 0, 3), (1, 0, 2, 3), (0, 0, 0, 1), (1, 0, 3, 2), (0, 0, 1, 0), (0, 1, 1, 2), (0, 1, 3, 0), (0, 1, 2, 1), (0, 1, 0, 3), (0, 1, 2, 3), (0, 1, 0, 1), (0, 1, 3, 2), (0, 1, 1, 0), (1, 1, 1, 2), (1, 1, 3, 0), (1, 1, 2, 1), (1, 1, 0, 3), (1, 1, 2, 3), (1, 1, 0, 1), (1, 1, 3, 2), (1, 1, 1, 0), (0, 1, 0, 2), (0, 1, 2, 0), (0, 1, 1, 1), (0, 1, 3, 3), (0, 1, 1, 3), (0, 1, 3, 1), (1, 1, 0, 2), (1, 1, 2, 0), (1, 1, 1, 1), (1, 1, 3, 3), (1, 1, 1, 3), (1, 1, 3, 1), (0, 0, 2, 2), (1, 0, 0, 0), (1, 0, 0, 2), (0, 0, 2, 0), (1, 0, 1, 1), (0, 0, 3, 3), (1, 0, 1, 3), (0, 0, 3, 1), (1, 0, 2, 0), (0, 0, 0, 2), (1, 0, 3, 1), (0, 0, 1, 3), (1, 0, 3, 3), (0, 0, 1, 1), (0, 0, 1, 2), (1, 0, 3, 0), (0, 0, 2, 1), (1, 0, 0, 3), (0, 0, 2, 3), (1, 0, 0, 1), (0, 0, 3, 2), (1, 0, 1, 0)]


FAR = sorted(ORDER, key=lambda s: -hops(s))


def kernel(
    x_ref, ig_ref, is_ref, wp_ref, wg_ref, og_ref, os_ref, wo_ref, out_ref,
    xin, xs, wall, lown, lsend, rsend, stage, recv_l, recv_r, psend, recv_p, recv_d, peer_p,
    gate, pn, ostage, wp, wg, wo, vecs,
    w_sem, own_sem, x_send, x_recv, l_send, l_recv, r_send, r_recv, p_send, p_recv, d_recv, e_send, e_recv,
):
    row = lax.axis_index("row")
    col = lax.axis_index("col")
    y = lax.axis_index("depth")
    zh, core = div(row, 2), rem(row, 2)
    zl, x = div(col, 4), rem(col, 4)
    q = col * 4 + y
    me = zh * 32 + q
    other = {"row": zh * 2 + 1 - core, "col": col, "depth": y}
    low = pl.multiple_of(zh * 384, 128)

    rows2 = [(zh, row, zh * 2 + 1 - core), (1 - zh, (1 - zh) * 2 + core, (1 - zh) * 2 + 1 - core)]
    xs2 = [rem(x + d, 4) for d in range(4)]
    cols2 = [[a * 4 + b for b in xs2] for a in (zl, 1 - zl)]
    ys2 = [rem(y + d, 4) for d in range(4)]

    def each_chip(use, order=ORDER):
        for dzh, dzl, dx, dy in order:
            zh2, row2, _ = rows2[dzh]
            q2 = cols2[dzl][dx] * 4 + ys2[dy]
            use(zh2, q2, zh2 * 32 + q2, {"row": row2, "col": cols2[dzl][dx], "depth": ys2[dy]})

    def each_device(use, order):
        for dzh, dzl, dx, dy in order:
            zh2, row2, cross2 = rows2[dzh]
            n = zh2 * 32 + cols2[dzl][dx] * 4 + ys2[dy]
            use(n, core, {"row": row2, "col": cols2[dzl][dx], "depth": ys2[dy]})
            use(n, 1 - core, {"row": cross2, "col": cols2[dzl][dx], "depth": ys2[dy]})
        use(me, 1 - core, other)

    weights = [
        pltpu.make_async_copy(src, dst, w_sem.at[n])
        for n, (src, dst) in enumerate(
            ((wp_ref, wp), (ig_ref, vecs.at[0]), (is_ref, vecs.at[1]), (wg_ref, wg), (og_ref, vecs.at[2]),
             (os_ref, vecs.at[3]), (wo_ref, wo))
        )
    ]

    def own_copy(t, u):
        start = core * 128 + u * 64 if u < 2 else 256 + core * 64
        return pltpu.make_async_copy(
            x_ref.at[:, u, :, pl.ds(t * 8, 8), :], xin.at[t, pl.ds(div(start, 8), 8)], own_sem.at[t]
        )

    for t in range(3):
        for u in range(3):
            own_copy(t, u).start()
    for copy in weights:
        copy.start()

    barrier = pltpu.get_barrier_semaphore()
    each_device(lambda n, owner, device: pl.semaphore_signal(barrier, inc=1, device_id=device), FAR)

    for copy in weights:
        copy.wait()
    for part in range(4):
        wall[part * 128 : (part + 1) * 128, :] = wp[:, part * 128 : (part + 1) * 128].astype(F32).T.astype(BF)

    in_gain = vecs[0]
    in_shift = vecs[1]
    mean_of = jnp.full((128, 128), 1.0 / 128.0, BF)
    mean_of_two = jnp.full((256, 128), 1.0 / 128.0, BF)

    def norm_own(t, carry):
        pltpu.make_async_copy(xin.at[t, pl.ds(0, 24)], xin.at[t, pl.ds(0, 24)], own_sem.at[t]).wait()
        for n in range(6):
            start = core * 16 + n * 4 if n < 4 else 32 + core * 8 + (n - 4) * 4
            raw = xin[t, pl.ds(start, 4)].reshape(256, 128)
            v = raw.astype(F32) - jnp.dot(raw, mean_of, preferred_element_type=F32)
            square = v * v
            upper = square.astype(BF)
            lower = (square - upper.astype(F32)).astype(BF)
            variance = jnp.dot(
                jnp.concatenate([upper, lower], axis=1), mean_of_two, preferred_element_type=F32
            )
            v = v * lax.rsqrt(variance + EPS) * in_gain + in_shift
            xs[pl.ds(pl.multiple_of(t * 3072 + start * 64, 256), 256), :] = v
            xin[t, pl.ds(start, 4)] = v.astype(BF).reshape(4, 8, 8, 128)
        return carry

    def group_of(t):
        late = div(t, 2)
        return div(q, 16) * 48 + rem(div(q, 8), 2) * (16 - 8 * late) + t * 8 * (1 - late) + 32 * late + rem(q, 8)

    norm_own(0, 0)
    for i in range(8):
        rows = xs[pl.ds(core * 1024 + i, 128, stride=8), :].astype(BF)
        p = dot_nt(wall[0:256, :], rows)
        pn[0, pl.ds(i, 128, stride=8), :] = jax.nn.sigmoid(p[0:128]) * p[128:256]
    lown[...] = pn[0].reshape(128, 8, 128).astype(BF)
    pl.semaphore_wait(barrier, 127)

    def peer_copy(t, u):
        here = pl.ds(core * 16, 16) if u == 0 else pl.ds(32 + core * 8, 8)
        return pltpu.make_async_remote_copy(
            src_ref=xin.at[t, here],
            dst_ref=xin.at[t, here],
            send_sem=x_send,
            recv_sem=x_recv.at[t],
            device_id=other,
        )

    def to_peer_rows(t):
        for u in range(2):
            peer_copy(t, u).start()

    to_peer_rows(0)

    own_tile = pl.ds(pl.multiple_of(zh * 384 + core * 128, 128), 128)
    group = group_of(jnp.int32(0))

    def send_own(n, owner, device):
        pltpu.make_async_remote_copy(
            src_ref=lown.at[owner * 64 + n],
            dst_ref=recv_l.at[group, :, own_tile],
            send_sem=l_send,
            recv_sem=l_recv,
            device_id=device,
        ).start()

    each_device(send_own, ORDER)
    recv_l[group, :, own_tile] = lown[core * 64 + me]

    def widen_peer(t):
        for n in range(6):
            start = (1 - core) * 16 + n * 4 if n < 4 else 32 + (1 - core) * 8 + (n - 4) * 4
            xs[pl.ds(pl.multiple_of(t * 3072 + start * 64, 256), 256), :] = (
                xin[t, pl.ds(start, 4)].reshape(256, 128).astype(F32)
            )

    def project(t, base, dst, tiles):
        w = jnp.concatenate(
            [wall[pl.ds(pl.multiple_of(part * 128 + core * 64, 64), 64), :] for part in (base, base + 1)], axis=0
        )
        for i in range(8):
            rows = xs[pl.ds(t * 3072 + tiles[0] * 1024 + i, len(tiles) * 128, stride=8), :].astype(BF)
            p = dot_nt(w, rows)
            side = jax.nn.sigmoid(p[0:64]) * p[64:128]
            for n, c in enumerate(tiles):
                stage[c, pl.ds(i, 64, stride=8), :] = side[:, n * 128 : (n + 1) * 128]
        for c in tiles:
            dst[pl.ds(t * 64, 64), :, c * 128 : (c + 1) * 128] = stage[c].reshape(64, 8, 128).astype(BF)

    def left(t, tiles):
        pltpu.make_async_copy(xin.at[t, pl.ds(0, 24)], xin.at[t, pl.ds(0, 24)], x_recv.at[t]).wait()
        widen_peer(t)
        project(t, 0, lsend, tiles)
        group = group_of(t)
        size = len(tiles) * 128
        src_lanes = pl.ds(tiles[0] * 128, size)
        dst_lanes = pl.ds(pl.multiple_of(low + tiles[0] * 128, 128), size)

        def send(zh2, q2, n, device):
            pltpu.make_async_remote_copy(
                src_ref=lsend.at[t * 64 + n, :, src_lanes],
                dst_ref=recv_l.at[group, :, dst_lanes],
                send_sem=l_send,
                recv_sem=l_recv,
                device_id=device,
            ).start()

        each_chip(send)
        recv_l[group, :, dst_lanes] = lsend[t * 64 + me, :, src_lanes]

    norm_own(1, 0)
    to_peer_rows(1)
    left(jnp.int32(0), (2,))
    norm_own(2, 0)
    to_peer_rows(2)

    def left_all(t, carry):
        left(t, (0, 1, 2))
        return carry

    lax.fori_loop(1, 3, left_all, 0)

    def right(t, carry):
        project(t, 2, rsend, (0, 1, 2))

        def send(zh2, q2, n, device):
            pltpu.make_async_remote_copy(
                src_ref=rsend.at[t * 64 + n],
                dst_ref=recv_r.at[t * 32 + q, :, pl.ds(low, 384)],
                send_sem=r_send,
                recv_sem=r_recv.at[t],
                device_id=device,
            ).start()

        each_chip(send)
        recv_r[t * 32 + q, :, pl.ds(low, 384)] = rsend[t * 64 + me]
        return carry

    lax.fori_loop(0, 3, right, 0)

    def gates(t, carry):
        w = wg[...]
        for i in range(8):
            a = xs[pl.ds(t * 3072 + core * 1024 + i, 128, stride=8), :].astype(BF)
            b = xs[pl.ds(t * 3072 + 2048 + core * 512 + i, 64, stride=8), :].astype(BF)
            rows = jnp.concatenate([a, b], axis=0)
            gate[t * 8 + i] = jax.nn.sigmoid(jnp.dot(rows, w, preferred_element_type=F32))
        return carry

    lax.fori_loop(0, 3, gates, 0)

    pltpu.make_async_copy(xs.at[pl.ds(0, 2272)], xs.at[pl.ds(0, 2272)], l_recv).wait()

    def product(t):
        pltpu.make_async_copy(rsend.at[pl.ds(0, 63)], rsend.at[pl.ds(0, 63)], r_recv.at[t]).wait()
        rows = recv_r[pl.ds(t * 32, 32)].reshape(256, 768)
        for part in range(3):
            cols = recv_l[pl.ds(part * 32, 32)].reshape(256, 768)
            psend[pl.ds(t * 32, 32), :, part * 256 : (part + 1) * 256] = (
                dot_nt(rows, cols).astype(BF).reshape(32, 8, 256)
            )

    def product_early(t, carry):
        product(t)

        def send(zh2, q2, n, device):
            pltpu.make_async_remote_copy(
                src_ref=psend.at[t * 32 + q2, :, pl.ds(pl.multiple_of(zh2 * 384, 128), 384)],
                dst_ref=recv_p.at[t * 64 + me],
                send_sem=p_send,
                recv_sem=p_recv.at[t],
                device_id=device,
            ).start()

        each_chip(send)
        recv_p[t * 64 + me] = psend[t * 32 + q, :, pl.ds(low, 384)]
        return carry

    lax.fori_loop(0, 2, product_early, 0)

    product(jnp.int32(2))
    shared = pl.ds(pl.multiple_of(low + 256, 128), 128)

    def send_shared(zh2, q2, n, device):
        pltpu.make_async_remote_copy(
            src_ref=psend.at[64 + q2, :, pl.ds(pl.multiple_of(zh2 * 384 + 256, 128), 128)],
            dst_ref=recv_p.at[128 + me, :, pl.ds(256, 128)],
            send_sem=p_send,
            recv_sem=p_recv.at[2],
            device_id=device,
        ).start()

    each_chip(send_shared)
    recv_p[128 + me, :, 256:384] = psend[64 + q, :, shared]

    def send_last(n, owner, device):
        lane = pl.multiple_of(div(n, 32) * 384 + owner * 128, 128)
        pltpu.make_async_remote_copy(
            src_ref=psend.at[64 + rem(n, 32), :, pl.ds(lane, 128)],
            dst_ref=recv_d.at[me if owner is core else 64 + me],
            send_sem=p_send,
            recv_sem=d_recv,
            device_id=device,
        ).start()

    each_device(send_last, ORDER)
    recv_d[me] = psend[64 + q, :, own_tile]

    def to_peer(t, half):
        lane = pl.multiple_of((1 - core) * 128, 128) if half == 0 else 256
        return pltpu.make_async_remote_copy(
            src_ref=recv_p.at[pl.ds(t * 64, 64), :, pl.ds(lane, 128)],
            dst_ref=peer_p.at[pl.ds(t * 64, 64), :, pl.ds(half * 128, 128)],
            send_sem=e_send,
            recv_sem=e_recv.at[t],
            device_id=other,
        )

    own_lane = pl.multiple_of(core * 128, 128)
    first = core == 0
    out_gain = jnp.where(first, vecs[2], pltpu.roll(vecs[2], 64, 1))
    out_shift = jnp.where(first, vecs[3], pltpu.roll(vecs[3], 64, 1))

    w_out = jnp.concatenate(
        [wo[pl.ds(pl.multiple_of(half * 64, 64), 64), :] for half in (core, 1 - core)], axis=0
    )

    def standardize(slot, read):
        total = jnp.zeros((8, 128), F32)
        for lo in range(0, 64, 16):
            a, b = read(lo, 16)
            total = total + (jnp.sum(a.astype(F32), axis=0) + jnp.sum(b.astype(F32), axis=0))
        average = (total * (1.0 / 128.0))[None]
        total = jnp.zeros((8, 128), F32)
        for lo in range(0, 64, 16):
            a, b = read(lo, 16)
            a, b = a.astype(F32) - average, b.astype(F32) - average
            total = total + (jnp.sum(a * a, axis=0) + jnp.sum(b * b, axis=0))
        scale = lax.rsqrt(total * (1.0 / 128.0) + EPS)[None]
        for lo in range(0, 64, 16):
            a, b = read(lo, 16)
            pn[slot, lo * 8 : lo * 8 + 128, :] = ((a.astype(F32) - average) * scale).reshape(128, 128)
            pn[slot, 512 + lo * 8 : 640 + lo * 8, :] = ((b.astype(F32) - average) * scale).reshape(128, 128)

    def project_out(t, slot):
        rows = 64 if slot else 128
        for j in range(8):
            v = pn[slot, pl.ds(j, 128, stride=8), :].T
            if slot:
                v = jnp.where(first, v[0:64], v[64:128])
            v = (v * out_gain + out_shift).astype(BF)
            u = jnp.dot(v, w_out, preferred_element_type=F32)
            ostage[pl.ds(slot * 1024 + j, rows, stride=8), :] = u * gate[t * 8 + j, slot * 128 : slot * 128 + rows]
        for u in ((2,) if slot else (0, 1)):
            out_ref[:, u, :, pl.ds(pl.multiple_of(t * 8, 8), 8), :] = (
                ostage[u * 512 : (u + 1) * 512, :].reshape(8, 8, 8, 128).astype(BF)
            )

    def read_shared(t):
        return lambda lo, size: (
            recv_p[pl.ds(t * 64 + lo, size), :, 256:384], peer_p[pl.ds(t * 64 + lo, size), :, 128:256]
        )

    def finish_early(t, carry):
        pltpu.make_async_copy(rsend.at[pl.ds(0, 63)], rsend.at[pl.ds(0, 63)], p_recv.at[t]).wait()
        to_peer(t, 0).start()
        to_peer(t, 1).start()
        pltpu.make_async_copy(peer_p.at[pl.ds(0, 64)], peer_p.at[pl.ds(0, 64)], e_recv.at[t]).wait()
        standardize(
            0,
            lambda lo, size: (
                recv_p[pl.ds(t * 64 + lo, size), :, pl.ds(own_lane, 128)], peer_p[pl.ds(t * 64 + lo, size), :, 0:128]
            ),
        )
        standardize(1, read_shared(t))
        project_out(t, 0)
        project_out(t, 1)
        return carry

    lax.fori_loop(0, 2, finish_early, 0)
    last = jnp.int32(2)
    pltpu.make_async_copy(lown.at[pl.ds(0, 63)], lown.at[pl.ds(0, 63)], p_recv.at[2]).wait()
    to_peer(last, 1).start()
    pltpu.make_async_copy(lown.at[pl.ds(0, 64)], lown.at[pl.ds(0, 64)], e_recv.at[2]).wait()
    standardize(1, read_shared(last))
    project_out(last, 1)
    pltpu.make_async_copy(lown.at[pl.ds(0, 127)], lown.at[pl.ds(0, 127)], d_recv).wait()
    standardize(0, lambda lo, size: (recv_d[lo : lo + size], recv_d[64 + lo : 64 + lo + size]))
    project_out(last, 0)

    for t in range(3):
        for u in range(2):
            peer_copy(t, u).wait_send()
        if t < 2:
            to_peer(t, 0).wait_send()
        to_peer(t, 1).wait_send()
    for sem in (l_send, p_send):
        pltpu.make_async_copy(xs.at[pl.ds(0, 2272)], xs.at[pl.ds(0, 2272)], sem).wait()
    pltpu.make_async_copy(rsend.at[pl.ds(0, 189)], rsend.at[pl.ds(0, 189)], r_send).wait()


def per_device(pair_input, in_gain, in_shift, w_proj, w_gate, out_gain, out_shift, w_out):
    vmem = pl.BlockSpec(memory_space=pltpu.VMEM)
    anyspace = pl.BlockSpec(memory_space=pltpu.HBM)
    dma = pltpu.SemaphoreType.DMA
    out = pl.pallas_call(
        kernel,
        out_shape=pltpu.VMEM((8, 3, 8, 24, 128), BF),
        in_specs=[anyspace] * 8,
        out_specs=vmem,
        scratch_shapes=[
            pltpu.VMEM((3, 48, 8, 8, 128), BF),
            pltpu.VMEM((9216, 128), F32),
            pltpu.VMEM((512, 128), BF),
            pltpu.VMEM((128, 8, 128), BF),
            pltpu.VMEM((192, 8, 384), BF),
            pltpu.VMEM((192, 8, 384), BF),
            pltpu.VMEM((3, 512, 128), F32),
            pltpu.VMEM((96, 8, 768), BF),
            pltpu.VMEM((96, 8, 768), BF),
            pltpu.VMEM((96, 8, 768), BF),
            pltpu.VMEM((192, 8, 384), BF),
            pltpu.VMEM((128, 8, 128), BF),
            pltpu.VMEM((192, 8, 256), BF),
            pltpu.VMEM((24, 192, 128), F32),
            pltpu.VMEM((2, 1024, 128), F32),
            pltpu.VMEM((1536, 128), F32),
            pltpu.VMEM((128, 512), BF),
            pltpu.VMEM((128, 128), BF),
            pltpu.VMEM((128, 128), BF),
            pltpu.VMEM((4, 1, 128), F32),
            dma((7,)),
            dma((3,)),
            dma,
            dma((3,)),
            dma,
            dma,
            dma,
            dma((3,)),
            dma,
            dma((3,)),
            dma,
            dma,
            dma((3,)),
        ],
        compiler_params=pltpu.CompilerParams(
            collective_id=0, has_side_effects=True, vmem_limit_bytes=int(54 * 2**20)
        ),
        name="triangle",
    )(
        *(
            pltpu.with_memory_space_constraint(a, pltpu.HBM)
            for a in (
                pair_input.reshape(8, 3, 8, 24, 128),
                in_gain.reshape(1, 128),
                in_shift.reshape(1, 128),
                w_proj,
                w_gate,
                out_gain.reshape(1, 128),
                out_shift.reshape(1, 128),
                w_out,
            )
        )
    )
    return out.reshape(192, 24, 128)


def solution(mesh):
    placed = (P("row", ("col", "depth"), None), P(), P(), P(), P(), P(), P(), P())
    return jax.shard_map(
        per_device,
        mesh=mesh,
        in_specs=placed,
        out_specs=P("row", ("col", "depth"), None),
        check_vma=False,
    )
```

```python
import itertools

import jax
import jax.numpy as jnp
from jax import lax
from jax.experimental import pallas as pl
from jax.experimental.pallas import tpu as pltpu
from jax.sharding import PartitionSpec as P

BF = jnp.bfloat16
F32 = jnp.float32
EPS = 1e-05


def div(a, b):
    return lax.div(a, jnp.int32(b))


def rem(a, b):
    return lax.rem(a, jnp.int32(b))


def dot_nt(a, b):
    return lax.dot_general(a, b, (((1,), (1,)), ((), ())), preferred_element_type=F32)


def hops(step):
    dzh, dzl, dx, dy = step
    return (2 if dzh else 0) + dzl + min(dx, 4 - dx) + min(dy, 4 - dy)


ORDER = [(1, 0, 2, 2), (0, 1, 2, 2), (0, 1, 0, 0), (1, 1, 2, 2), (1, 1, 0, 0), (1, 0, 1, 2), (0, 0, 3, 0), (1, 0, 2, 1), (0, 0, 0, 3), (1, 0, 2, 3), (0, 0, 0, 1), (1, 0, 3, 2), (0, 0, 1, 0), (0, 1, 1, 2), (0, 1, 3, 0), (0, 1, 2, 1), (0, 1, 0, 3), (0, 1, 2, 3), (0, 1, 0, 1), (0, 1, 3, 2), (0, 1, 1, 0), (1, 1, 1, 2), (1, 1, 3, 0), (1, 1, 2, 1), (1, 1, 0, 3), (1, 1, 2, 3), (1, 1, 0, 1), (1, 1, 3, 2), (1, 1, 1, 0), (0, 1, 0, 2), (0, 1, 2, 0), (0, 1, 1, 1), (0, 1, 3, 3), (0, 1, 1, 3), (0, 1, 3, 1), (1, 1, 0, 2), (1, 1, 2, 0), (1, 1, 1, 1), (1, 1, 3, 3), (1, 1, 1, 3), (1, 1, 3, 1), (0, 0, 2, 2), (1, 0, 0, 0), (1, 0, 0, 2), (0, 0, 2, 0), (1, 0, 1, 1), (0, 0, 3, 3), (1, 0, 1, 3), (0, 0, 3, 1), (1, 0, 2, 0), (0, 0, 0, 2), (1, 0, 3, 1), (0, 0, 1, 3), (1, 0, 3, 3), (0, 0, 1, 1), (0, 0, 1, 2), (1, 0, 3, 0), (0, 0, 2, 1), (1, 0, 0, 3), (0, 0, 2, 3), (1, 0, 0, 1), (0, 0, 3, 2), (1, 0, 1, 0)]


FAR = sorted(ORDER, key=lambda s: -hops(s))


def kernel(
    x_ref, ig_ref, is_ref, wp_ref, wg_ref, og_ref, os_ref, wo_ref, out_ref,
    xin, xs, wall, lown, lsend, rsend, stage, recv_l, recv_r, psend, recv_p, recv_d, peer_p,
    gate, pn, ostage, wp, wg, wo, vecs,
    w_sem, own_sem, x_send, x_recv, l_send, l_recv, r_send, r_recv, p_send, p_recv, d_recv, e_send, e_recv, ready,
):
    row = lax.axis_index("row")
    col = lax.axis_index("col")
    y = lax.axis_index("depth")
    zh, core = div(row, 2), rem(row, 2)
    zl, x = div(col, 4), rem(col, 4)
    q = col * 4 + y
    me = zh * 32 + q
    other = {"row": zh * 2 + 1 - core, "col": col, "depth": y}
    low = pl.multiple_of(zh * 384, 128)

    rows2 = [(zh, row, zh * 2 + 1 - core), (1 - zh, (1 - zh) * 2 + core, (1 - zh) * 2 + 1 - core)]
    xs2 = [rem(x + d, 4) for d in range(4)]
    cols2 = [[a * 4 + b for b in xs2] for a in (zl, 1 - zl)]
    ys2 = [rem(y + d, 4) for d in range(4)]

    def each_chip(use, order=ORDER):
        for dzh, dzl, dx, dy in order:
            zh2, row2, _ = rows2[dzh]
            q2 = cols2[dzl][dx] * 4 + ys2[dy]
            use(zh2, q2, zh2 * 32 + q2, {"row": row2, "col": cols2[dzl][dx], "depth": ys2[dy]})

    def each_device(use, order):
        for dzh, dzl, dx, dy in order:
            zh2, row2, cross2 = rows2[dzh]
            n = zh2 * 32 + cols2[dzl][dx] * 4 + ys2[dy]
            use(n, core, {"row": row2, "col": cols2[dzl][dx], "depth": ys2[dy]})
            use(n, 1 - core, {"row": cross2, "col": cols2[dzl][dx], "depth": ys2[dy]})
        use(me, 1 - core, other)

    weights = [
        pltpu.make_async_copy(src, dst, w_sem.at[n])
        for n, (src, dst) in enumerate(
            ((wp_ref, wp), (ig_ref, vecs.at[0]), (is_ref, vecs.at[1]), (wg_ref, wg), (og_ref, vecs.at[2]),
             (os_ref, vecs.at[3]), (wo_ref, wo))
        )
    ]

    def own_copy(t, u):
        start = core * 128 + u * 64 if u < 2 else 256 + core * 64
        return pltpu.make_async_copy(
            x_ref.at[:, u, :, pl.ds(t * 8, 8), :], xin.at[t, pl.ds(div(start, 8), 8)], own_sem.at[t]
        )

    for t in range(3):
        for u in range(3):
            own_copy(t, u).start()
    for copy in weights:
        copy.start()

    barrier = pltpu.get_barrier_semaphore()
    each_chip(lambda zh2, q2, n, device: pl.semaphore_signal(barrier, inc=1, device_id=device), FAR)
    pl.semaphore_signal(barrier, inc=1, device_id=other)

    for n in (1, 2):
        weights[n].wait()

    in_gain = vecs[0]
    in_shift = vecs[1]
    mean_of = jnp.full((128, 128), 1.0 / 128.0, BF)
    mean_of_two = jnp.full((256, 128), 1.0 / 128.0, BF)

    def norm_own(t, carry):
        pltpu.make_async_copy(xin.at[t, pl.ds(0, 24)], xin.at[t, pl.ds(0, 24)], own_sem.at[t]).wait()
        for n in range(6):
            start = core * 16 + n * 4 if n < 4 else 32 + core * 8 + (n - 4) * 4
            raw = xin[t, pl.ds(start, 4)].reshape(256, 128)
            v = raw.astype(F32) - jnp.dot(raw, mean_of, preferred_element_type=F32)
            square = v * v
            upper = square.astype(BF)
            lower = (square - upper.astype(F32)).astype(BF)
            variance = jnp.dot(
                jnp.concatenate([upper, lower], axis=1), mean_of_two, preferred_element_type=F32
            )
            v = v * lax.rsqrt(variance + EPS) * in_gain + in_shift
            xs[pl.ds(pl.multiple_of(t * 3072 + start * 64, 256), 256), :] = v
            xin[t, pl.ds(start, 4)] = v.astype(BF).reshape(4, 8, 8, 128)
        return carry

    def group_of(t):
        late = div(t, 2)
        return div(q, 16) * 48 + rem(div(q, 8), 2) * (16 - 8 * late) + t * 8 * (1 - late) + 32 * late + rem(q, 8)

    norm_own(0, 0)
    def turn(part):
        wall[part * 128 : (part + 1) * 128, :] = wp[:, part * 128 : (part + 1) * 128].astype(F32).T.astype(BF)

    weights[0].wait()
    turn(0)
    turn(1)
    for i in range(8):
        rows = xs[pl.ds(core * 1024 + i, 128, stride=8), :].astype(BF)
        p = dot_nt(wall[0:256, :], rows)
        pn[0, pl.ds(i, 128, stride=8), :] = jax.nn.sigmoid(p[0:128]) * p[128:256]
    lown[...] = pn[0].reshape(128, 8, 128).astype(BF)
    pl.semaphore_wait(barrier, 64)
    pl.semaphore_signal(ready, inc=1, device_id=other)

    def peer_copy(t, u):
        here = pl.ds(core * 16, 16) if u == 0 else pl.ds(32 + core * 8, 8)
        return pltpu.make_async_remote_copy(
            src_ref=xin.at[t, here],
            dst_ref=xin.at[t, here],
            send_sem=x_send,
            recv_sem=x_recv.at[t],
            device_id=other,
        )

    def to_peer_rows(t):
        for u in range(2):
            peer_copy(t, u).start()

    to_peer_rows(0)

    own_tile = pl.ds(pl.multiple_of(zh * 384 + core * 128, 128), 128)
    group = group_of(jnp.int32(0))

    def send_own(n, owner, device):
        pltpu.make_async_remote_copy(
            src_ref=lown.at[owner * 64 + n],
            dst_ref=recv_l.at[group, :, own_tile],
            send_sem=l_send,
            recv_sem=l_recv,
            device_id=device,
        ).start()

    each_chip(lambda zh2, q2, n, device: send_own(n, core, device))
    pl.semaphore_wait(ready, 1)
    each_device(lambda n, owner, device: send_own(n, owner, device) if owner is not core else None, ORDER)
    recv_l[group, :, own_tile] = lown[core * 64 + me]

    def widen_peer(t):
        for n in range(6):
            start = (1 - core) * 16 + n * 4 if n < 4 else 32 + (1 - core) * 8 + (n - 4) * 4
            xs[pl.ds(pl.multiple_of(t * 3072 + start * 64, 256), 256), :] = (
                xin[t, pl.ds(start, 4)].reshape(256, 128).astype(F32)
            )

    def project(t, base, dst, tiles):
        w = jnp.concatenate(
            [wall[pl.ds(pl.multiple_of(part * 128 + core * 64, 64), 64), :] for part in (base, base + 1)], axis=0
        )
        for i in range(8):
            rows = xs[pl.ds(t * 3072 + tiles[0] * 1024 + i, len(tiles) * 128, stride=8), :].astype(BF)
            p = dot_nt(w, rows)
            side = jax.nn.sigmoid(p[0:64]) * p[64:128]
            for n, c in enumerate(tiles):
                stage[c, pl.ds(i, 64, stride=8), :] = side[:, n * 128 : (n + 1) * 128]
        for c in tiles:
            dst[pl.ds(t * 64, 64), :, c * 128 : (c + 1) * 128] = stage[c].reshape(64, 8, 128).astype(BF)

    def left(t, tiles):
        pltpu.make_async_copy(xin.at[t, pl.ds(0, 24)], xin.at[t, pl.ds(0, 24)], x_recv.at[t]).wait()
        widen_peer(t)
        project(t, 0, lsend, tiles)
        group = group_of(t)
        size = len(tiles) * 128
        src_lanes = pl.ds(tiles[0] * 128, size)
        dst_lanes = pl.ds(pl.multiple_of(low + tiles[0] * 128, 128), size)

        def send(zh2, q2, n, device):
            pltpu.make_async_remote_copy(
                src_ref=lsend.at[t * 64 + n, :, src_lanes],
                dst_ref=recv_l.at[group, :, dst_lanes],
                send_sem=l_send,
                recv_sem=l_recv,
                device_id=device,
            ).start()

        each_chip(send)
        recv_l[group, :, dst_lanes] = lsend[t * 64 + me, :, src_lanes]

    norm_own(1, 0)
    to_peer_rows(1)
    left(jnp.int32(0), (2,))
    norm_own(2, 0)
    to_peer_rows(2)

    def left_all(t, carry):
        left(t, (0, 1, 2))
        return carry

    lax.fori_loop(1, 3, left_all, 0)

    turn(2)
    turn(3)
    for n in (3, 4, 5, 6):
        weights[n].wait()

    def right(t, carry):
        project(t, 2, rsend, (0, 1, 2))

        def send(zh2, q2, n, device):
            pltpu.make_async_remote_copy(
                src_ref=rsend.at[t * 64 + n],
                dst_ref=recv_r.at[t * 32 + q, :, pl.ds(low, 384)],
                send_sem=r_send,
                recv_sem=r_recv.at[t],
                device_id=device,
            ).start()

        each_chip(send)
        recv_r[t * 32 + q, :, pl.ds(low, 384)] = rsend[t * 64 + me]
        return carry

    lax.fori_loop(0, 3, right, 0)

    def gates(t, carry):
        w = wg[...]
        for i in range(8):
            a = xs[pl.ds(t * 3072 + core * 1024 + i, 128, stride=8), :].astype(BF)
            b = xs[pl.ds(t * 3072 + 2048 + core * 512 + i, 64, stride=8), :].astype(BF)
            rows = jnp.concatenate([a, b], axis=0)
            gate[t * 8 + i] = jax.nn.sigmoid(jnp.dot(rows, w, preferred_element_type=F32))
        return carry

    lax.fori_loop(0, 3, gates, 0)

    pltpu.make_async_copy(xs.at[pl.ds(0, 2272)], xs.at[pl.ds(0, 2272)], l_recv).wait()

    def product(t):
        pltpu.make_async_copy(rsend.at[pl.ds(0, 63)], rsend.at[pl.ds(0, 63)], r_recv.at[t]).wait()
        rows = recv_r[pl.ds(t * 32, 32)].reshape(256, 768)
        for part in range(3):
            cols = recv_l[pl.ds(part * 32, 32)].reshape(256, 768)
            psend[pl.ds(t * 32, 32), :, part * 256 : (part + 1) * 256] = (
                dot_nt(rows, cols).astype(BF).reshape(32, 8, 256)
            )

    def product_early(t, carry):
        product(t)

        def send(zh2, q2, n, device):
            pltpu.make_async_remote_copy(
                src_ref=psend.at[t * 32 + q2, :, pl.ds(pl.multiple_of(zh2 * 384, 128), 384)],
                dst_ref=recv_p.at[t * 64 + me],
                send_sem=p_send,
                recv_sem=p_recv.at[t],
                device_id=device,
            ).start()

        each_chip(send)
        recv_p[t * 64 + me] = psend[t * 32 + q, :, pl.ds(low, 384)]
        return carry

    lax.fori_loop(0, 2, product_early, 0)

    product(jnp.int32(2))
    shared = pl.ds(pl.multiple_of(low + 256, 128), 128)

    def send_shared(zh2, q2, n, device):
        pltpu.make_async_remote_copy(
            src_ref=psend.at[64 + q2, :, pl.ds(pl.multiple_of(zh2 * 384 + 256, 128), 128)],
            dst_ref=recv_p.at[128 + me, :, pl.ds(256, 128)],
            send_sem=p_send,
            recv_sem=p_recv.at[2],
            device_id=device,
        ).start()

    each_chip(send_shared)
    recv_p[128 + me, :, 256:384] = psend[64 + q, :, shared]

    def send_last(n, owner, device):
        lane = pl.multiple_of(div(n, 32) * 384 + owner * 128, 128)
        pltpu.make_async_remote_copy(
            src_ref=psend.at[64 + rem(n, 32), :, pl.ds(lane, 128)],
            dst_ref=recv_d.at[me if owner is core else 64 + me],
            send_sem=p_send,
            recv_sem=d_recv,
            device_id=device,
        ).start()

    each_device(send_last, ORDER)
    recv_d[me] = psend[64 + q, :, own_tile]

    def to_peer(t, half):
        lane = pl.multiple_of((1 - core) * 128, 128) if half == 0 else 256
        return pltpu.make_async_remote_copy(
            src_ref=recv_p.at[pl.ds(t * 64, 64), :, pl.ds(lane, 128)],
            dst_ref=peer_p.at[pl.ds(t * 64, 64), :, pl.ds(half * 128, 128)],
            send_sem=e_send,
            recv_sem=e_recv.at[t],
            device_id=other,
        )

    own_lane = pl.multiple_of(core * 128, 128)
    first = core == 0
    out_gain = jnp.where(first, vecs[2], pltpu.roll(vecs[2], 64, 1))
    out_shift = jnp.where(first, vecs[3], pltpu.roll(vecs[3], 64, 1))

    w_out = jnp.concatenate(
        [wo[pl.ds(pl.multiple_of(half * 64, 64), 64), :] for half in (core, 1 - core)], axis=0
    )

    def standardize(slot, read):
        total = jnp.zeros((8, 128), F32)
        for lo in range(0, 64, 16):
            a, b = read(lo, 16)
            total = total + (jnp.sum(a.astype(F32), axis=0) + jnp.sum(b.astype(F32), axis=0))
        average = (total * (1.0 / 128.0))[None]
        total = jnp.zeros((8, 128), F32)
        for lo in range(0, 64, 16):
            a, b = read(lo, 16)
            a, b = a.astype(F32) - average, b.astype(F32) - average
            total = total + (jnp.sum(a * a, axis=0) + jnp.sum(b * b, axis=0))
        scale = lax.rsqrt(total * (1.0 / 128.0) + EPS)[None]
        for lo in range(0, 64, 16):
            a, b = read(lo, 16)
            pn[slot, lo * 8 : lo * 8 + 128, :] = ((a.astype(F32) - average) * scale).reshape(128, 128)
            pn[slot, 512 + lo * 8 : 640 + lo * 8, :] = ((b.astype(F32) - average) * scale).reshape(128, 128)

    def project_out(t, slot):
        rows = 64 if slot else 128
        for j in range(8):
            v = pn[slot, pl.ds(j, 128, stride=8), :].T
            if slot:
                v = jnp.where(first, v[0:64], v[64:128])
            v = (v * out_gain + out_shift).astype(BF)
            u = jnp.dot(v, w_out, preferred_element_type=F32)
            ostage[pl.ds(slot * 1024 + j, rows, stride=8), :] = u * gate[t * 8 + j, slot * 128 : slot * 128 + rows]
        for u in ((2,) if slot else (0, 1)):
            out_ref[:, u, :, pl.ds(pl.multiple_of(t * 8, 8), 8), :] = (
                ostage[u * 512 : (u + 1) * 512, :].reshape(8, 8, 8, 128).astype(BF)
            )

    def read_shared(t):
        return lambda lo, size: (
            recv_p[pl.ds(t * 64 + lo, size), :, 256:384], peer_p[pl.ds(t * 64 + lo, size), :, 128:256]
        )

    def finish_early(t, carry):
        pltpu.make_async_copy(rsend.at[pl.ds(0, 63)], rsend.at[pl.ds(0, 63)], p_recv.at[t]).wait()
        to_peer(t, 0).start()
        to_peer(t, 1).start()
        pltpu.make_async_copy(peer_p.at[pl.ds(0, 64)], peer_p.at[pl.ds(0, 64)], e_recv.at[t]).wait()
        standardize(
            0,
            lambda lo, size: (
                recv_p[pl.ds(t * 64 + lo, size), :, pl.ds(own_lane, 128)], peer_p[pl.ds(t * 64 + lo, size), :, 0:128]
            ),
        )
        standardize(1, read_shared(t))
        project_out(t, 0)
        project_out(t, 1)
        return carry

    lax.fori_loop(0, 2, finish_early, 0)
    last = jnp.int32(2)
    pltpu.make_async_copy(lown.at[pl.ds(0, 63)], lown.at[pl.ds(0, 63)], p_recv.at[2]).wait()
    to_peer(last, 1).start()
    pltpu.make_async_copy(lown.at[pl.ds(0, 64)], lown.at[pl.ds(0, 64)], e_recv.at[2]).wait()
    standardize(1, read_shared(last))
    project_out(last, 1)
    pltpu.make_async_copy(lown.at[pl.ds(0, 127)], lown.at[pl.ds(0, 127)], d_recv).wait()
    standardize(0, lambda lo, size: (recv_d[lo : lo + size], recv_d[64 + lo : 64 + lo + size]))
    project_out(last, 0)

    for t in range(3):
        for u in range(2):
            peer_copy(t, u).wait_send()
        if t < 2:
            to_peer(t, 0).wait_send()
        to_peer(t, 1).wait_send()
    for sem in (l_send, p_send):
        pltpu.make_async_copy(xs.at[pl.ds(0, 2272)], xs.at[pl.ds(0, 2272)], sem).wait()
    pltpu.make_async_copy(rsend.at[pl.ds(0, 189)], rsend.at[pl.ds(0, 189)], r_send).wait()


def per_device(pair_input, in_gain, in_shift, w_proj, w_gate, out_gain, out_shift, w_out):
    vmem = pl.BlockSpec(memory_space=pltpu.VMEM)
    anyspace = pl.BlockSpec(memory_space=pltpu.HBM)
    dma = pltpu.SemaphoreType.DMA
    out = pl.pallas_call(
        kernel,
        out_shape=pltpu.VMEM((8, 3, 8, 24, 128), BF),
        in_specs=[anyspace] * 8,
        out_specs=vmem,
        scratch_shapes=[
            pltpu.VMEM((3, 48, 8, 8, 128), BF),
            pltpu.VMEM((9216, 128), F32),
            pltpu.VMEM((512, 128), BF),
            pltpu.VMEM((128, 8, 128), BF),
            pltpu.VMEM((192, 8, 384), BF),
            pltpu.VMEM((192, 8, 384), BF),
            pltpu.VMEM((3, 512, 128), F32),
            pltpu.VMEM((96, 8, 768), BF),
            pltpu.VMEM((96, 8, 768), BF),
            pltpu.VMEM((96, 8, 768), BF),
            pltpu.VMEM((192, 8, 384), BF),
            pltpu.VMEM((128, 8, 128), BF),
            pltpu.VMEM((192, 8, 256), BF),
            pltpu.VMEM((24, 192, 128), F32),
            pltpu.VMEM((2, 1024, 128), F32),
            pltpu.VMEM((1536, 128), F32),
            pltpu.VMEM((128, 512), BF),
            pltpu.VMEM((128, 128), BF),
            pltpu.VMEM((128, 128), BF),
            pltpu.VMEM((4, 1, 128), F32),
            dma((7,)),
            dma((3,)),
            dma,
            dma((3,)),
            dma,
            dma,
            dma,
            dma((3,)),
            dma,
            dma((3,)),
            dma,
            dma,
            dma((3,)),
            pltpu.SemaphoreType.REGULAR,
        ],
        compiler_params=pltpu.CompilerParams(
            collective_id=0, has_side_effects=True, vmem_limit_bytes=int(54 * 2**20)
        ),
        name="triangle",
    )(
        *(
            pltpu.with_memory_space_constraint(a, pltpu.HBM)
            for a in (
                pair_input.reshape(8, 3, 8, 24, 128),
                in_gain.reshape(1, 128),
                in_shift.reshape(1, 128),
                w_proj,
                w_gate,
                out_gain.reshape(1, 128),
                out_shift.reshape(1, 128),
                w_out,
            )
        )
    )
    return out.reshape(192, 24, 128)


def solution(mesh):
    placed = (P("row", ("col", "depth"), None), P(), P(), P(), P(), P(), P(), P())
    return jax.shard_map(
        per_device,
        mesh=mesh,
        in_specs=placed,
        out_specs=P("row", ("col", "depth"), None),
        check_vma=False,
    )
```
